128 devices in a mesh: band: 16 (over x, y_hi, core), grid: 8 (over y_lo, z).
Axes of the slice: x: 4, y: 4 (y_hi: 2, y_lo: 2; y = y_hi * 2 + y_lo), z: 4, core: 2. Of those that a mesh axis runs over, the one named last changes fastest.
Arguments:
- wave: bfloat16 [4096, 20480], P('band', 'grid'), may hold values from -6 to 6
- ritz: bfloat16 [4096, 4096], P('band', 'grid'), may hold values from -0.125 to 0.125
- occupation: float32 [4096], P('band'), may hold values from 0 to 2
Outputs:
- rotated: bfloat16 [4096, 20480], P('band', 'grid')
- density: float32 [20480], P('grid')
The draws below stay inside these ranges and needn't reach their ends.
All inputs are finite; a program needn't handle non-finite values.
Results may differ from the reference program's by a relative error of at most 0.0017.
Values may be sent and summed in bfloat16 or wider, within the bound.
A program may use at most 128 MiB of HBM per device.

```python
import jax
import jax.numpy as jnp
from jax import lax

NB = 4096
CELLS = 20480


def strengthened(values, stream_key, source, target, blocks, factor):
    def block_of(position):
        return (jnp.arange(values.shape[position]) // (values.shape[position] // blocks)).reshape((-1,) + (1,) * (values.ndim - 1 - position))

    first = jax.random.permutation(stream_key, blocks)[block_of(target)]
    other_side = (block_of(target) + blocks // 2) % blocks
    return jnp.where((block_of(source) == first) | (block_of(source) == other_side), factor * values, values)


def shard_levels(rng, extent, pieces, low, high):
    factor_of = 1.0
    for axis_at, blocks in pieces:
        heights = jax.random.uniform(jax.random.fold_in(jax.random.fold_in(rng, 6), axis_at), (blocks,), jnp.float32, low / len(pieces), high / len(pieces))
        factor_of = factor_of * jnp.repeat(jnp.exp(heights), extent[axis_at] // blocks).reshape((-1,) + (1,) * (len(extent) - 1 - axis_at))
    return factor_of


def bell_draw(rng, extent, deviation, most, cuts=(), held_as=jnp.bfloat16):
    array = jax.random.normal(rng, extent, jnp.float32) * deviation
    if len(cuts) > 0:
        array = shard_levels(rng, extent, cuts, -0.22, 0.18) * array
    return jnp.clip(array, min=-most, max=most).astype(held_as)


def gaussian_with(rng, shape, spread, reach, shards, heavy, held_as=jnp.bfloat16):
    entries = spread * jax.random.normal(rng, shape, jnp.float32)
    if shards:
        entries = entries * shard_levels(rng, shape, shards, -0.22, 0.18)
    return jnp.clip(strengthened(entries, jax.random.fold_in(rng, 3), *heavy), -reach, reach).astype(held_as)


def setup_inputs(seed: int = 0) -> dict:
    keys = jax.random.split(jax.random.key(seed), 4)
    return {
        "wave": bell_draw(keys[0], (NB, CELLS), 1.0, 6.0, ((0, 16), (1, 8))),
        "ritz": gaussian_with(keys[1], (NB, NB), NB ** -0.5, 0.125, ((0, 16), (1, 8)), (0, 1, 16, 2.0)),
        "occupation": jnp.clip(2.0 * jax.random.uniform(keys[2], (NB,), jnp.float32) ** shard_levels(keys[2], (NB,), ((0, 16),), -0.2, 0.2), 0.0, 2.0),
    }


def reference(wave, ritz, occupation):
    summed = jnp.dot(ritz.astype(jnp.float32).T, wave.astype(jnp.float32), precision=lax.Precision.HIGHEST)
    rotated = summed.astype(jnp.bfloat16)
    values = rotated.astype(jnp.float32)
    density = jnp.sum(occupation[:, None] * values * values, axis=0) / NB
    return rotated, density
```

```python
import jax
import jax.numpy as jnp
from jax import lax
from jax.experimental import pallas as pl
from jax.experimental.pallas import tpu as pltpu
from jax.sharding import PartitionSpec as P

NB = 4096
MESH = pl.DeviceIdType.MESH
F32, BF16 = jnp.float32, jnp.bfloat16

NK = 5
SLABS = 4

N_RINGS = 13


def at(x, y, z, core):
    return (x * 4 + (y // 2) * 2 + core, (y % 2) * 4 + z)


def kernel(
    wave, ritz, occ, out, dens,
    rt_src, stage, rt, w, cbuf, occ_rows, occ_cols, dpart, dsend, dslot,
    sa_send, sa_recv, s0_send, s0_recv, s1_send, s1_recv, ring_send, ring_recv,
    core_send, core_recv, occ_send, occ_recv, c_send, c_recv, d_send, d_recv,
):
    band, grid = lax.axis_index("band"), lax.axis_index("grid")
    x, yhi, c = band // 4, (band // 2) % 2, band % 2
    ylo, z = grid // 4, grid % 4
    y = yhi * 2 + ylo
    xj = 2 * ylo + z // 2
    zb = z % 2
    mine = yhi * 2 + c

    def half_of(yy):
        return (yy // 2 + yy % 2 + 1) % 2

    def send(src, dst, send_sem, recv_sem, device):
        return pltpu.make_async_remote_copy(
            src_ref=src, dst_ref=dst, send_sem=send_sem, recv_sem=recv_sem,
            device_id=device, device_id_type=MESH,
        )

    rt_src[...] = ritz[...].T.reshape(2, 4, 4, 16, 256)
    occ_rows[mine] = occ[...]

    def scatter(d):
        p = (z * 4 + y + d) % 16
        zp, yp = p // 4, p % 4
        return send(
            rt_src.at[:, zp, yp],
            stage.at[xj, pl.ds(zb * 2, 2), :, pl.ds(pl.multiple_of(yhi * 256, 256), 256)],
            s0_send.at[d], s0_recv.at[d], at(x, yp, zp, c),
        )

    def scatter_in(d):
        p = (z * 4 + y - d + 16) % 16
        zp, yp = p // 4, p % 4
        return send(
            rt_src.at[:, zp, yp],
            stage.at[2 * (yp % 2) + zp // 2, pl.ds((zp % 2) * 2, 2), :,
                     pl.ds(pl.multiple_of((yp // 2) * 256, 256), 256)],
            s0_send.at[d], s0_recv.at[d], at(x, yp, zp, c),
        )

    def wave_copy(k, j):
        up, core = j // 2, j % 2
        yy = (y + 1) % 4 if up else (y + 3) % 4
        col = pl.multiple_of(half_of(yy) * 1280 + core * 640 + k * 128, 128)
        return send(
            wave.at[:, pl.ds(col, 128)],
            w.at[k, c, pl.ds(pl.multiple_of(x * 512 + yhi * 256, 256), 256), :],
            sa_send.at[k, j], sa_recv.at[k], at(x, yy, z, core),
        )

    def wave_in(k):
        rows = w.at[k, :, pl.ds(pl.multiple_of(x * 512, 512), 512), :]
        return send(rows, rows, sa_send.at[k, 0], sa_recv.at[k], at(x, y, z, c))

    def ring(i):
        if i < 5:
            me, plus, minus = x, at((x + 1) % 4, y, z, c), at((x + 3) % 4, y, z, c)
            block = lambda v, h: w.at[i, h, pl.ds(pl.multiple_of(v * 512, 512), 512), :]
        elif i < 8:
            me, plus, minus = y, at(x, (y + 1) % 4, z, c), at(x, (y + 3) % 4, z, c)
            block = lambda v, h: rt.at[c, i - 5, z, v, :, pl.ds(h * 1024, 1024)]
        elif i < 11:
            me, plus, minus = z, at(x, y, (z + 1) % 4, c), at(x, y, (z + 3) % 4, c)
            block = lambda v, h: rt.at[c, i - 8, v, pl.ds(h * 2, 2)]
        elif i == 11:
            me, plus, minus = z, at(x, y, (z + 1) % 4, c), at(x, y, (z + 3) % 4, c)
            block = lambda v, h: rt.at[c, 3, v, y, :, pl.ds(h * 1024, 1024)]
        else:
            me, plus, minus = y, at(x, (y + 1) % 4, z, c), at(x, (y + 3) % 4, z, c)
            block = lambda v, h: rt.at[c, 3, pl.ds(h * 2, 2), v]

        def copy(j, v, h):
            ref = block((me + v) % 4, h)
            return send(ref, ref, ring_send.at[i, j], ring_recv.at[i, j], plus if j < 3 else minus)

        return copy

    def own(i):
        copy = ring(i)
        copy(0, 0, 0).start()
        copy(3, 0, 1).start()
        copy(1, 0, 1).start()
        copy(4, 0, 0).start()

    def relay(i):
        copy = ring(i)
        copy(0, 3, 0).wait_recv()
        copy(2, 3, 0).start()
        copy(3, 1, 1).wait_recv()
        copy(5, 1, 1).start()

    def finish(i):
        copy = ring(i)
        copy(1, 3, 1).wait_recv()
        copy(4, 1, 0).wait_recv()
        copy(2, 2, 0).wait_recv()
        copy(5, 2, 1).wait_recv()

    def drain(i):
        copy = ring(i)
        for j, v, h in ((0, 0, 0), (3, 0, 1), (1, 0, 1), (4, 0, 0), (2, 3, 0), (5, 1, 1)):
            copy(j, v, h).wait_send()

    def spread(d):
        to = (x + d) % 4
        return send(
            stage.at[to],
            rt.at[c, :, z, y, :, pl.ds(pl.multiple_of(x * 512, 512), 512)],
            s1_send.at[d], s1_recv.at[d], at(to, y, z, c),
        )

    def spread_in(d):
        src = (x - d + 4) % 4
        return send(
            stage.at[src],
            rt.at[c, :, z, y, :, pl.ds(pl.multiple_of(src * 512, 512), 512)],
            s1_send.at[d], s1_recv.at[d], at(src, y, z, c),
        )

    def to_partner(s):
        return send(rt.at[c, s], rt.at[c, s], core_send.at[s], core_recv.at[s], at(x, y, z, 1 - c))

    def from_partner(s):
        return send(rt.at[1 - c, s], rt.at[1 - c, s], core_send.at[s], core_recv.at[s], at(x, y, z, 1 - c))

    def occ_copy(d):
        yy = y if d == 0 else (y + 2) % 4
        cc = c if d == 1 else 1 - c
        return send(occ, occ_rows.at[mine], occ_send.at[d], occ_recv.at[d], at(x, yy, z, cc))

    def occ_in(d):
        hi = yhi if d == 0 else 1 - yhi
        cc = c if d == 1 else 1 - c
        return send(occ, occ_rows.at[hi * 2 + cc], occ_send.at[d], occ_recv.at[d], at(x, y, z, 1 - c))

    def result_copy(k, s):
        col = pl.multiple_of(half_of(y) * 1280 + c * 640 + k * 128, 128)
        return send(
            cbuf.at[k, s], out.at[:, pl.ds(col, 128)],
            c_send.at[k, s], c_recv.at[0], at(x, 2 * (s // 2) + 1 - ylo, z, s % 2),
        )

    def density_copy(d):
        return send(
            dsend, dslot.at[x * 4 + half_of(y) * 2 + c], d_send.at[d], d_recv.at[0],
            at(d // 4, 2 * ((d // 2) % 2) + 1 - ylo, z, d % 2),
        )

    for d in range(1, 16):
        scatter(d).start()
    for k in range(2):
        for j in range(4):
            wave_copy(k, j).start()
    for d in range(3):
        occ_copy(d).start()
    stage[xj, pl.ds(zb * 2, 2), :, pl.ds(pl.multiple_of(yhi * 256, 256), 256)] = rt_src[:, z, y]

    wave_in(0).wait_recv()
    own(0)
    for d in range(1, 16):
        scatter_in(d).wait_recv()
    for d in range(1, 4):
        spread(d).start()
    rt[c, :, z, y, :, pl.ds(pl.multiple_of(x * 512, 512), 512)] = stage[x]
    wave_in(1).wait_recv()
    own(1)
    for d in range(1, 4):
        spread_in(d).wait_recv()
    for i in (5, 6, 7, 11):
        own(i)
    for k in range(2, NK):
        for j in range(4):
            wave_copy(k, j).start()
    relay(0)
    for i in (5, 6, 7, 11):
        relay(i)
    for i in (5, 6, 7):
        finish(i)
        own(i + 3)
    finish(11)
    own(12)
    relay(1)
    wave_in(2).wait_recv()
    own(2)
    for d in range(3):
        occ_in(d).wait_recv()
    for s in range(SLABS):
        occ_cols[s] = jnp.broadcast_to(occ_rows[s][0:1, :], (128, 256)).T
    relay(8)
    wave_in(3).wait_recv()
    own(3)
    relay(12)
    relay(9)
    wave_in(4).wait_recv()
    own(4)
    relay(2)
    finish(8)
    to_partner(0).start()
    relay(10)
    relay(3)
    finish(9)
    to_partner(1).start()
    finish(12)
    to_partner(3).start()
    finish(10)
    to_partner(2).start()
    relay(4)
    for s in range(SLABS):
        from_partner(s).wait_recv()

    dpart[...] = jnp.zeros_like(dpart)
    for k in range(NK):
        finish(k)

        @pl.loop(0, SLABS)
        def _(s):
            summed = jnp.dot(
                rt[0, s].reshape(256, 2048), w[k, 0], preferred_element_type=F32
            ) + jnp.dot(rt[1, s].reshape(256, 2048), w[k, 1], preferred_element_type=F32)
            rounded = summed.astype(BF16)
            cbuf[k, s] = rounded
            values = rounded.astype(F32)
            terms = occ_cols[s] * values * values
            dpart[k] += terms.reshape(32, 8, 128).sum(axis=0)
            result_copy(k, s).start()

    dsend[...] = jnp.zeros_like(dsend)
    for k in range(NK):
        dsend[k : k + 1, :] = jnp.sum(dpart[k], axis=0, keepdims=True)
    for d in range(16):
        density_copy(d).start()

    for d in range(1, 16):
        scatter(d).wait_send()
    for k in range(NK):
        for j in range(4):
            wave_copy(k, j).wait_send()
    for d in range(1, 4):
        spread(d).wait_send()
    for i in range(N_RINGS):
        drain(i)
    for s in range(SLABS):
        to_partner(s).wait_send()
    for d in range(3):
        occ_copy(d).wait_send()

    send(dslot, dslot, d_send.at[0], d_recv.at[0], at(x, y, z, c)).wait_recv()
    for g in range(4):
        total = dslot[g] + dslot[4 + g] + dslot[8 + g] + dslot[12 + g]
        dens[g * NK : (g + 1) * NK, :] = total[:NK] * (1.0 / NB)

    send(out, out, c_send.at[0, 0], c_recv.at[0], at(x, y, z, c)).wait_recv()
    for k in range(NK):
        for s in range(SLABS):
            result_copy(k, s).wait_send()
    for d in range(16):
        density_copy(d).wait_send()


def per_device(wave, ritz, occupation):
    occ = jnp.broadcast_to(occupation.reshape(1, 256), (8, 256))
    dma = pltpu.SemaphoreType.DMA
    vmem = pl.BlockSpec(memory_space=pltpu.VMEM)
    anywhere = pl.BlockSpec(memory_space=pl.ANY)
    rotated, density = pl.pallas_call(
        kernel,
        out_shape=(
            jax.ShapeDtypeStruct((256, 2560), BF16),
            jax.ShapeDtypeStruct((20, 128), F32),
        ),
        in_specs=[anywhere, vmem, vmem],
        out_specs=(anywhere, vmem),
        scratch_shapes=[
            pltpu.VMEM((2, 4, 4, 16, 256), BF16),
            pltpu.VMEM((4, 4, 16, 512), BF16),
            pltpu.VMEM((2, 4, 4, 4, 16, 2048), BF16),
            pltpu.VMEM((NK, 2, 2048, 128), BF16),
            pltpu.VMEM((NK, 4, 256, 128), BF16),
            pltpu.VMEM((4, 8, 256), F32),
            pltpu.VMEM((4, 256, 128), F32),
            pltpu.VMEM((NK, 8, 128), F32),
            pltpu.VMEM((8, 128), F32),
            pltpu.VMEM((16, 8, 128), F32),
            dma((NK, 4)), dma((NK,)),
            dma((16,)), dma((16,)),
            dma((4,)), dma((4,)),
            dma((N_RINGS, 6)), dma((N_RINGS, 6)),
            dma((4,)), dma((4,)),
            dma((3,)), dma((3,)),
            dma((NK, 4)), dma((1,)),
            dma((16,)), dma((1,)),
        ],
        compiler_params=pltpu.CompilerParams(
            has_side_effects=True, vmem_limit_bytes=60 * 1024 * 1024
        ),
        name="rotate",
    )(wave, ritz, occ)
    return rotated, density.reshape(2560)


def solution(mesh):
    return jax.shard_map(
        per_device,
        mesh=mesh,
        in_specs=(P("band", "grid"), P("band", "grid"), P("band")),
        out_specs=(P("band", "grid"), P("grid")),
        check_vma=False,
    )
```

```python
import jax
import jax.numpy as jnp
from jax import lax
from jax.experimental import pallas as pl
from jax.experimental.pallas import tpu as pltpu
from jax.sharding import PartitionSpec as P

NB = 4096
MESH = pl.DeviceIdType.MESH
F32, BF16 = jnp.float32, jnp.bfloat16

NK = 5
SLABS = 4

N_RINGS = 13


def at(x, y, z, core):
    return (x * 4 + (y // 2) * 2 + core, (y % 2) * 4 + z)


def kernel(
    wave, ritz, occ, out, dens,
    rt_src, stage, rt, w, cbuf, occ_rows, occ_cols, dpart, dsend, dslot,
    sa_send, sa_recv, s0_send, s0_recv, s1_send, s1_recv, ring_send, ring_recv,
    core_send, core_recv, occ_send, occ_recv, c_send, c_recv, d_send, d_recv,
):
    band, grid = lax.axis_index("band"), lax.axis_index("grid")
    x, yhi, c = band // 4, (band // 2) % 2, band % 2
    ylo, z = grid // 4, grid % 4
    y = yhi * 2 + ylo
    xj = 2 * ylo + z // 2
    zb = z % 2
    mine = yhi * 2 + c

    def half_of(yy):
        return (yy // 2 + yy % 2 + 1) % 2

    def send(src, dst, send_sem, recv_sem, device):
        return pltpu.make_async_remote_copy(
            src_ref=src, dst_ref=dst, send_sem=send_sem, recv_sem=recv_sem,
            device_id=device, device_id_type=MESH,
        )

    peers = [at(x, ((z * 4 + y + d) % 16) % 4, ((z * 4 + y + d) % 16) // 4, c) for d in range(1, 16)]
    peers += [at((x + d) % 4, y, z, c) for d in range(1, 4)]
    peers += [at(x, (y + d) % 4, z, 1 - c) for d in range(4)]
    peers += [
        at((x + d) % 4, (y + e) % 4, z, f) for d in range(1, 4) for e in (1, 3) for f in range(2)
    ]
    barrier = pltpu.get_barrier_semaphore()
    with jax.named_scope("signal"):
        for peer in peers:
            pl.semaphore_signal(barrier, inc=1, device_id=peer, device_id_type=MESH)

    with jax.named_scope("transpose"):
        rt_src[...] = ritz[...].T.reshape(2, 4, 4, 16, 256)
        occ_rows[mine] = jnp.broadcast_to(occ[...], (8, 256))
    with jax.named_scope("barrier"):
        pl.semaphore_wait(barrier, len(peers))

    def scatter(d):
        p = (z * 4 + y + d) % 16
        zp, yp = p // 4, p % 4
        return send(
            rt_src.at[:, zp, yp],
            stage.at[xj, pl.ds(zb * 2, 2), :, pl.ds(pl.multiple_of(yhi * 256, 256), 256)],
            s0_send.at[d], s0_recv.at[d], at(x, yp, zp, c),
        )

    def scatter_in(d):
        p = (z * 4 + y - d + 16) % 16
        zp, yp = p // 4, p % 4
        return send(
            rt_src.at[:, zp, yp],
            stage.at[2 * (yp % 2) + zp // 2, pl.ds((zp % 2) * 2, 2), :,
                     pl.ds(pl.multiple_of((yp // 2) * 256, 256), 256)],
            s0_send.at[d], s0_recv.at[d], at(x, yp, zp, c),
        )

    def cells(k):
        return pl.ds((k % 2) * 128, 128)

    def wave_copy(k, j):
        up, core = j // 2, j % 2
        yy = (y + 1) % 4 if up else (y + 3) % 4
        col = pl.multiple_of(half_of(yy) * 1280 + core * 640 + k * 128, 128)
        return send(
            wave.at[:, pl.ds(col, 128)],
            w.at[k // 2, c, pl.ds(pl.multiple_of(x * 512 + yhi * 256, 256), 256), cells(k)],
            sa_send.at[k, j], sa_recv.at[k], at(x, yy, z, core),
        )

    def wave_in(k):
        rows = w.at[k // 2, :, pl.ds(pl.multiple_of(x * 512, 512), 512), cells(k)]
        return send(rows, rows, sa_send.at[k, 0], sa_recv.at[k], at(x, y, z, c))

    def ring(i):
        if i < 5:
            me, plus, minus = x, at((x + 1) % 4, y, z, c), at((x + 3) % 4, y, z, c)
            block = lambda v, h: w.at[i // 2, h, pl.ds(pl.multiple_of(v * 512, 512), 512), cells(i)]
        elif i < 8:
            me, plus, minus = y, at(x, (y + 1) % 4, z, c), at(x, (y + 3) % 4, z, c)
            block = lambda v, h: rt.at[c, i - 5, z, v, :, pl.ds(h * 1024, 1024)]
        elif i < 11:
            me, plus, minus = z, at(x, y, (z + 1) % 4, c), at(x, y, (z + 3) % 4, c)
            block = lambda v, h: rt.at[c, i - 8, v, pl.ds(h * 2, 2)]
        elif i == 11:
            me, plus, minus = z, at(x, y, (z + 1) % 4, c), at(x, y, (z + 3) % 4, c)
            block = lambda v, h: rt.at[c, 3, v, y, :, pl.ds(h * 1024, 1024)]
        else:
            me, plus, minus = y, at(x, (y + 1) % 4, z, c), at(x, (y + 3) % 4, z, c)
            block = lambda v, h: rt.at[c, 3, pl.ds(h * 2, 2), v]

        def copy(j, v, h):
            ref = block((me + v) % 4, h)
            return send(ref, ref, ring_send.at[i, j], ring_recv.at[i, j], plus if j < 3 else minus)

        return copy

    def own(i):
        copy = ring(i)
        copy(0, 0, 0).start()
        copy(3, 0, 1).start()
        copy(1, 0, 1).start()
        copy(4, 0, 0).start()

    def relay(i):
        copy = ring(i)
        copy(0, 3, 0).wait_recv()
        copy(2, 3, 0).start()
        copy(3, 1, 1).wait_recv()
        copy(5, 1, 1).start()

    def finish(i):
        copy = ring(i)
        copy(1, 3, 1).wait_recv()
        copy(4, 1, 0).wait_recv()
        copy(2, 2, 0).wait_recv()
        copy(5, 2, 1).wait_recv()

    def drain(i):
        copy = ring(i)
        for j, v, h in ((0, 0, 0), (3, 0, 1), (1, 0, 1), (4, 0, 0), (2, 3, 0), (5, 1, 1)):
            copy(j, v, h).wait_send()

    def spread(d):
        to = (x + d) % 4
        return send(
            stage.at[to],
            rt.at[c, :, z, y, :, pl.ds(pl.multiple_of(x * 512, 512), 512)],
            s1_send.at[d], s1_recv.at[d], at(to, y, z, c),
        )

    def spread_in(d):
        src = (x - d + 4) % 4
        return send(
            stage.at[src],
            rt.at[c, :, z, y, :, pl.ds(pl.multiple_of(src * 512, 512), 512)],
            s1_send.at[d], s1_recv.at[d], at(src, y, z, c),
        )

    def to_partner(s):
        return send(rt.at[c, s], rt.at[c, s], core_send.at[s], core_recv.at[s], at(x, y, z, 1 - c))

    def from_partner(s):
        return send(rt.at[1 - c, s], rt.at[1 - c, s], core_send.at[s], core_recv.at[s], at(x, y, z, 1 - c))

    def occ_copy(d):
        yy = y if d == 0 else (y + 2) % 4
        cc = c if d == 1 else 1 - c
        return send(occ_rows.at[mine], occ_rows.at[mine], occ_send.at[d], occ_recv.at[d], at(x, yy, z, cc))

    def occ_in(d):
        hi = yhi if d == 0 else 1 - yhi
        cc = c if d == 1 else 1 - c
        return send(occ_rows.at[mine], occ_rows.at[hi * 2 + cc], occ_send.at[d], occ_recv.at[d], at(x, y, z, 1 - c))

    def result_copy(k, s):
        col = pl.multiple_of(half_of(y) * 1280 + c * 640 + k * 128, 128)
        return send(
            cbuf.at[k, s], out.at[:, pl.ds(col, 128)],
            c_send.at[k, s], c_recv.at[0], at(x, 2 * (s // 2) + 1 - ylo, z, s % 2),
        )

    def density_copy(d):
        return send(
            dsend, dslot.at[x * 4 + half_of(y) * 2 + c], d_send.at[d], d_recv.at[0],
            at(d // 4, 2 * ((d // 2) % 2) + 1 - ylo, z, d % 2),
        )

    def send_wave(k):
        for j in range(4):
            wave_copy(k, j).start()

    def slab(v, s):
        return rt[v, s].reshape(256, 2048)

    def take(k, s, summed):
        rounded = summed.astype(BF16)
        cbuf[k, s] = rounded
        values = rounded.astype(F32)
        terms = occ_cols[s] * values * values
        dpart[k] += terms.reshape(32, 8, 128).sum(axis=0)

    def wide(pair, s):
        summed = jnp.dot(slab(0, s), w[pair, 0], preferred_element_type=F32)
        summed += jnp.dot(slab(1, s), w[pair, 1], preferred_element_type=F32)
        for n in range(2):
            take(2 * pair + n, s, summed[:, n * 128 : (n + 1) * 128])
        for n in range(2):
            result_copy(2 * pair + n, s).start()

    def narrow(s):
        summed = jnp.dot(slab(0, s), w[2, 0, :, :128], preferred_element_type=F32)
        summed += jnp.dot(slab(1, s), w[2, 1, :, :128], preferred_element_type=F32)
        take(4, s, summed)
        result_copy(4, s).start()

    def all_slabs(body):
        @pl.loop(0, SLABS)
        def _(t):
            body((t % 2) * 2 + t // 2)

    with jax.named_scope("start"):
        for d in range(1, 16):
            scatter(d).start()
        send_wave(0)
        send_wave(1)
        for d in range(3):
            occ_copy(d).start()
        stage[xj, pl.ds(zb * 2, 2), :, pl.ds(pl.multiple_of(yhi * 256, 256), 256)] = rt_src[:, z, y]
    with jax.named_scope("scatter_in"):
        for d in range(1, 16):
            scatter_in(d).wait_recv()
    with jax.named_scope("spread"):
        for d in range(1, 4):
            spread(d).start()
        rt[c, :, z, y, :, pl.ds(pl.multiple_of(x * 512, 512), 512)] = stage[x]
    with jax.named_scope("wave0"):
        wave_in(0).wait_recv()
        own(0)
    with jax.named_scope("spread_in"):
        for d in range(1, 4):
            spread_in(d).wait_recv()
        own(5)
        own(6)
        own(7)
        own(11)
        send_wave(2)
    with jax.named_scope("wave1"):
        wave_in(1).wait_recv()
        own(1)
    with jax.named_scope("occ"):
        for d in range(3):
            occ_in(d).wait_recv()
        for s in range(SLABS):
            occ_cols[s] = jnp.broadcast_to(occ_rows[s][0:1, :], (128, 256)).T
        dpart[...] = jnp.zeros_like(dpart)
    with jax.named_scope("relay5"):
        relay(5)
        relay(6)
        relay(7)
        relay(11)
    with jax.named_scope("finish5"):
        finish(5)
        own(8)
    with jax.named_scope("finish6"):
        finish(6)
        own(9)
    with jax.named_scope("finish11"):
        finish(11)
        own(12)
    with jax.named_scope("relay0"):
        relay(0)
        send_wave(3)
    with jax.named_scope("finish7"):
        finish(7)
    with jax.named_scope("wave2"):
        wave_in(2).wait_recv()
        own(2)
    with jax.named_scope("relay8"):
        relay(8)
        own(10)
    with jax.named_scope("relay12"):
        relay(12)
        send_wave(4)
    with jax.named_scope("relay1"):
        relay(1)
    with jax.named_scope("wave3"):
        wave_in(3).wait_recv()
        own(3)
    with jax.named_scope("relay9"):
        relay(9)
    with jax.named_scope("finish8"):
        finish(8)
        to_partner(0).start()
    with jax.named_scope("finish12"):
        finish(12)
        to_partner(3).start()
    with jax.named_scope("relay10"):
        relay(10)
    with jax.named_scope("relay2"):
        relay(2)
    with jax.named_scope("wave4"):
        wave_in(4).wait_recv()
        own(4)
    with jax.named_scope("finish9"):
        finish(9)
        to_partner(1).start()
    with jax.named_scope("finish0"):
        finish(0)
        finish(1)
    with jax.named_scope("slab0"):
        from_partner(0).wait_recv()
        wide(0, 0)
    with jax.named_scope("slab3"):
        from_partner(3).wait_recv()
        wide(0, 3)
    with jax.named_scope("finish10"):
        finish(10)
        to_partner(2).start()
    with jax.named_scope("relay3"):
        relay(3)
    with jax.named_scope("slab1"):
        from_partner(1).wait_recv()
        wide(0, 1)
    with jax.named_scope("slab2"):
        from_partner(2).wait_recv()
        wide(0, 2)
    with jax.named_scope("finish2"):
        finish(2)
    with jax.named_scope("finish3"):
        finish(3)
    with jax.named_scope("relay4"):
        relay(4)
    with jax.named_scope("pair1"):
        all_slabs(lambda s: wide(1, s))
    with jax.named_scope("finish4"):
        finish(4)
    with jax.named_scope("last"):
        all_slabs(narrow)

    with jax.named_scope("density"):
        dsend[...] = jnp.zeros_like(dsend)
        for k in range(NK):
            dsend[k : k + 1, :] = jnp.sum(dpart[k], axis=0, keepdims=True)
        for d in range(16):
            density_copy(d).start()

    with jax.named_scope("drain"):
        for d in range(1, 16):
            scatter(d).wait_send()
        for k in range(NK):
            for j in range(4):
                wave_copy(k, j).wait_send()
        for d in range(1, 4):
            spread(d).wait_send()
        for i in range(N_RINGS):
            drain(i)
        for s in range(SLABS):
            to_partner(s).wait_send()
        for d in range(3):
            occ_copy(d).wait_send()

    with jax.named_scope("density_in"):
        send(dslot, dslot, d_send.at[0], d_recv.at[0], at(x, y, z, c)).wait_recv()
        for g in range(4):
            total = dslot[g] + dslot[4 + g] + dslot[8 + g] + dslot[12 + g]
            dens[g * NK : (g + 1) * NK, :] = total[:NK] * (1.0 / NB)

    with jax.named_scope("out_in"):
        send(out, out, c_send.at[0, 0], c_recv.at[0], at(x, y, z, c)).wait_recv()
    with jax.named_scope("out_sent"):
        for k in range(NK):
            for s in range(SLABS):
                result_copy(k, s).wait_send()
        for d in range(16):
            density_copy(d).wait_send()


def per_device(wave, ritz, occupation):
    occ = occupation.reshape(1, 256)
    dma = pltpu.SemaphoreType.DMA
    vmem = pl.BlockSpec(memory_space=pltpu.VMEM)
    anywhere = pl.BlockSpec(memory_space=pl.ANY)
    rotated, density = pl.pallas_call(
        kernel,
        out_shape=(
            jax.ShapeDtypeStruct((256, 2560), BF16),
            jax.ShapeDtypeStruct((20, 128), F32),
        ),
        in_specs=[anywhere, vmem, vmem],
        out_specs=(anywhere, vmem),
        scratch_shapes=[
            pltpu.VMEM((2, 4, 4, 16, 256), BF16),
            pltpu.VMEM((4, 4, 16, 512), BF16),
            pltpu.VMEM((2, 4, 4, 4, 16, 2048), BF16),
            pltpu.VMEM((3, 2, 2048, 256), BF16),
            pltpu.VMEM((NK, 4, 256, 128), BF16),
            pltpu.VMEM((4, 8, 256), F32),
            pltpu.VMEM((4, 256, 128), F32),
            pltpu.VMEM((NK, 8, 128), F32),
            pltpu.VMEM((8, 128), F32),
            pltpu.VMEM((16, 8, 128), F32),
            dma((NK, 4)), dma((NK,)),
            dma((16,)), dma((16,)),
            dma((4,)), dma((4,)),
            dma((N_RINGS, 6)), dma((N_RINGS, 6)),
            dma((4,)), dma((4,)),
            dma((3,)), dma((3,)),
            dma((NK, 4)), dma((1,)),
            dma((16,)), dma((1,)),
        ],
        compiler_params=pltpu.CompilerParams(
            has_side_effects=True, collective_id=0, vmem_limit_bytes=60 * 1024 * 1024
        ),
        name="rotate",
    )(wave, ritz, occ)
    return rotated, density.reshape(2560)


def solution(mesh):
    return jax.shard_map(
        per_device,
        mesh=mesh,
        in_specs=(P("band", "grid"), P("band", "grid"), P("band")),
        out_specs=(P("band", "grid"), P("grid")),
        check_vma=False,
    )
```

```python
import jax
import jax.numpy as jnp
from jax import lax
from jax.experimental import pallas as pl
from jax.experimental.pallas import tpu as pltpu
from jax.sharding import PartitionSpec as P

NB = 4096
MESH = pl.DeviceIdType.MESH
F32, BF16 = jnp.float32, jnp.bfloat16

NK = 5
CA = 1536

N_RINGS = 16

PARTNER_WAVE, FAR_WAVE, SCATTER, SPREAD, RING_X, RING_YZ, CORE, OCC, RESULT, DENSITY, LOCAL = range(11)
OWN_RESULT = RING_X


def at(x, y, z, core):
    return (x * 4 + (y // 2) * 2 + core, (y % 2) * 4 + z)


def kernel(
    wave, ritz, occ, out, dens,
    rt_src, stage, rt, w, cbuf, occ_rows, occ_cols, dpart, dsend, dslot,
    out_sem, in_sem, wave_sem, ring_sem, half_sem,
):
    band, grid = lax.axis_index("band"), lax.axis_index("grid")
    x, yhi, c = band // 4, (band // 2) % 2, band % 2
    ylo, z = grid // 4, grid % 4
    y = yhi * 2 + ylo
    xj = 2 * ylo + z // 2
    zb = z % 2
    mine = yhi * 2 + c
    near, far = yhi, 1 - yhi

    def many(n, i):
        return pl.ds(pl.multiple_of(i * n, n), n)

    def send(src, dst, send_sem, recv_sem, device):
        return pltpu.make_async_remote_copy(
            src_ref=src, dst_ref=dst, send_sem=send_sem, recv_sem=recv_sem,
            device_id=device, device_id_type=MESH,
        )

    def cells(k):
        return pl.ds((k % 2) * 128, 128)

    def wave_local(p):
        width = 256 if p < 2 else 128
        col = pl.multiple_of(yhi * 1280 + c * 640 + p * 256, 128)
        return pltpu.make_async_copy(
            wave.at[:, pl.ds(col, width)],
            w.at[p, c, many(256, x * 2 + near), pl.ds(0, width)],
            in_sem.at[LOCAL],
        )

    def wave_partner(p):
        width = 256 if p < 2 else 128
        col = pl.multiple_of(yhi * 1280 + (1 - c) * 640 + p * 256, 128)
        return send(
            wave.at[:, pl.ds(col, width)],
            w.at[p, c, many(256, x * 2 + near), pl.ds(0, width)],
            out_sem.at[PARTNER_WAVE], in_sem.at[PARTNER_WAVE], at(x, y, z, 1 - c),
        )

    def wave_far(k, core):
        col = pl.multiple_of((1 - yhi) * 1280 + core * 640 + k * 128, 128)
        return send(
            wave.at[:, pl.ds(col, 128)],
            w.at[k // 2, c, many(256, x * 2 + near), cells(k)],
            out_sem.at[FAR_WAVE], wave_sem.at[k], at(x, (y + 2) % 4, z, core),
        )

    def wave_in(k):
        rows = w.at[k // 2, :, many(256, x * 2 + far), cells(k)]
        return send(rows, rows, out_sem.at[FAR_WAVE], wave_sem.at[k], at(x, (y + 2) % 4, z, c))

    def scatter(d, src):
        p = (z * 4 + y + (16 - d if src else d)) % 16
        zp, yp = p // 4, p % 4
        ys, zs = (yp, zp) if src else (y, z)
        return send(
            rt_src.at[:, zp, yp],
            stage.at[2 * (ys % 2) + zs // 2, many(2, zs % 2), :, many(256, ys // 2)],
            out_sem.at[SCATTER], in_sem.at[SCATTER], at(x, yp, zp, c),
        )

    def spread(d, src):
        other = (x + (4 - d if src else d)) % 4
        return send(
            stage.at[other], rt.at[c, :, z, y, :, many(512, other if src else x)],
            out_sem.at[SPREAD], in_sem.at[SPREAD], at(other, y, z, c),
        )

    def ring(i):
        if i < 10:
            k, rows = i % 5, (near if i < 5 else far)
            block = lambda v, h: w.at[k // 2, h, many(256, v * 2 + rows), cells(k)]
        elif i == 10:
            block = lambda v, h: rt.at[c, :, z, v, :, pl.ds(h * (CA // 2), CA // 2)]
        elif i == 11:
            n = (2048 - CA) // 2
            block = lambda v, h: rt.at[c, :, v, y, :, pl.ds(CA + h * n, n)]
        elif i < 14:
            block = lambda v, h: rt.at[c, pl.ds((i - 12) * 2, 2), v, pl.ds(h * 2, 2), :, pl.ds(0, CA)]
        else:
            n = 2048 - CA
            block = lambda v, h: rt.at[c, pl.ds((i - 14) * 2, 2), pl.ds(h * 2, 2), v, :, pl.ds(CA, n)]
        return block, i

    def ring_copy(i, j, v, h):
        if isinstance(i, tuple):
            half = i[1]
            block = lambda v, h: rt.at[c, many(2, half), v, pl.ds(h * 2, 2), :, pl.ds(0, CA)]
            axis, slot = "z", 12 + half
        else:
            block, slot = ring(i)
            axis = "x" if i < 10 else "z" if i in (11, 12, 13) else "y"
        to = 1 if j < 3 else 3
        if axis == "x":
            me, device = x, at((x + to) % 4, y, z, c)
        elif axis == "y":
            me, device = y, at(x, (y + to) % 4, z, c)
        else:
            me, device = z, at(x, y, (z + to) % 4, c)
        ref = block((me + v) % 4, h)
        sent = out_sem.at[RING_X if axis == "x" else RING_YZ]
        if j in (0, 3):
            got = ring_sem.at[slot, j // 3]
        elif axis == "x":
            got = half_sem.at[2 + max(slot % 5 - 1, 0)]
        else:
            got = ring_sem.at[slot, 2]
        return send(ref, ref, sent, got, device)

    def own(i):
        ring_copy(i, 0, 0, 0).start()
        ring_copy(i, 3, 0, 1).start()
        ring_copy(i, 1, 0, 1).start()
        ring_copy(i, 4, 0, 0).start()

    def relay(i):
        ring_copy(i, 0, 3, 0).wait_recv()
        ring_copy(i, 2, 3, 0).start()
        ring_copy(i, 3, 1, 1).wait_recv()
        ring_copy(i, 5, 1, 1).start()

    def bytes_in(ref, sem):
        send(ref, ref, out_sem.at[0], sem, at(x, y, z, 1 - c)).wait_recv()

    def bytes_out(ref, sem):
        send(ref, ref, sem, in_sem.at[0], at(x, y, z, 1 - c)).wait_send()

    def finish(i):
        if isinstance(i, tuple):
            bytes_in(rt.at[c, many(2, i[1]), pl.ds(0, 2), :, :, pl.ds(0, CA)], ring_sem.at[12 + i[1], 2])
        elif i == 10:
            bytes_in(rt.at[c, :, 0, pl.ds(0, 2), :, pl.ds(0, CA)], ring_sem.at[i, 2])
        elif i == 11:
            bytes_in(rt.at[c, :, pl.ds(0, 2), 0, :, pl.ds(CA, 2048 - CA)], ring_sem.at[i, 2])
        else:
            bytes_in(rt.at[c, pl.ds((i - 14) * 2, 2), :, pl.ds(0, 2), :, pl.ds(CA, 2048 - CA)], ring_sem.at[i, 2])

    def finish_wave(g):
        bytes_in(w.at[0, :, pl.ds(0, 512 if g else 1024), :], half_sem.at[2 + g])

    zfar, znear = (0, far), (0, near)

    def partner(half, part, src=False):
        cc = 1 - c if src else c
        cols = pl.ds(0, CA) if part == 0 else pl.ds(CA, 2048 - CA)
        ref = rt.at[cc, many(2, half), :, :, :, cols]
        return send(ref, ref, out_sem.at[CORE], half_sem.at[half], at(x, y, z, 1 - c))

    def occ_copy(d, src=False):
        yy = y if d == 0 else (y + 2) % 4
        cc = c if d == 1 else 1 - c
        row = (yy // 2) * 2 + cc if src else mine
        return send(
            occ_rows.at[mine], occ_rows.at[row], out_sem.at[OCC], in_sem.at[OCC], at(x, yy, z, cc)
        )

    def result(k, hi, core):
        return send(
            cbuf.at[k, hi * 2 + core], out.at[:, many(128, yhi * 10 + c * 5 + k)],
            out_sem.at[RESULT], in_sem.at[RESULT], at(x, hi * 2 + ylo, z, core),
        )

    def result_here(k):
        return pltpu.make_async_copy(
            cbuf.at[k, mine], out.at[:, many(128, yhi * 10 + c * 5 + k)], in_sem.at[OWN_RESULT]
        )

    def density_copy(d):
        to = at((x + d // 4) % 4, (y + 2 * ((d // 2) % 2)) % 4, z, (c + d) % 2)
        return send(dsend, dslot.at[band], out_sem.at[DENSITY], in_sem.at[DENSITY], to)

    def take(k, s, summed):
        rounded = summed.astype(BF16)
        cbuf[k, s] = rounded
        values = rounded.astype(F32)
        terms = occ_cols[s] * values * values
        dpart[k] += terms.reshape(32, 8, 128).sum(axis=0)

    def product(s, ks):
        cols = pl.ds((ks[0] % 2) * 128, 128 * len(ks))
        parts = [
            jnp.dot(
                rt[v, s].reshape(256, 2048), w[ks[0] // 2, v, :, cols], preferred_element_type=F32
            )
            for v in range(2)
        ]
        return parts[0] + parts[1]

    def blocks(ks, hi):
        @pl.loop(0, 2)
        def _(core):
            s = hi * 2 + core
            summed = product(s, ks)
            for n, k in enumerate(ks):
                take(k, s, summed[:, n * 128 : (n + 1) * 128])
            if hi is far:
                for k in ks:
                    result(k, hi, core).start()

        if hi is near:
            for k in ks:
                result(k, hi, 1 - c).start()
            for k in ks:
                result_here(k).start()

    with jax.named_scope("signal"):
        for p in range(3):
            wave_local(p).start()
        peers = []
        for d in range(1, 16):
            p = (z * 4 + y + d) % 16
            peers.append(at(x, p % 4, p // 4, c))
        for d in range(1, 16):
            if d != 2:
                peers.append(at((x + d // 4) % 4, (y + 2 * ((d // 2) % 2)) % 4, z, (c + d) % 2))
        barrier = pltpu.get_barrier_semaphore()
        for peer in peers:
            pl.semaphore_signal(barrier, inc=1, device_id=peer, device_id_type=MESH)

    with jax.named_scope("transpose"):
        rt_src[...] = ritz[...].T.reshape(2, 4, 4, 16, 256)
        occ_rows[mine] = jnp.broadcast_to(occ[...], (8, 256))
        stage[xj, many(2, zb), :, many(256, yhi)] = rt_src[:, z, y]
        dpart[...] = jnp.zeros_like(dpart)
        dsend[...] = jnp.zeros_like(dsend)
    with jax.named_scope("barrier"):
        pl.semaphore_wait(barrier, len(peers))

    with jax.named_scope("start"):
        for d in range(1, 16):
            scatter(d, 0).start()
        few = wave.at[:, pl.ds(0, 640)]
        pltpu.make_async_copy(few, few, in_sem.at[LOCAL]).wait()
        for p in range(3):
            wave_partner(p).start()
        for d in range(3):
            occ_copy(d).start()
    with jax.named_scope("pw"):
        bytes_in(wave.at[:, pl.ds(0, 640)], in_sem.at[PARTNER_WAVE])
        own(0)
    with jax.named_scope("scin"):
        bytes_in(w.at[0, 0, pl.ds(0, 480), :], in_sem.at[SCATTER])
        for d in range(1, 4):
            spread(d, 0).start()
        rt[c, :, z, y, :, many(512, x)] = stage[x]
        for core in range(2):
            wave_far(0, core).start()
        for core in range(2):
            wave_far(1, core).start()
        own(1)
        own(2)
        own(3)
    with jax.named_scope("spin"):
        bytes_in(stage.at[pl.ds(0, 3)], in_sem.at[SPREAD])
        own(10)
        own(11)
    with jax.named_scope("occ"):
        bytes_in(occ_rows.at[pl.ds(0, 3)], in_sem.at[OCC])
        for s in range(4):
            occ_cols[s] = jnp.broadcast_to(occ_rows[s][0:1, :], (128, 256)).T
    with jax.named_scope("s1relay"):
        relay(10)
        relay(11)
    with jax.named_scope("relay0"):
        relay(0)
    with jax.named_scope("wave0"):
        wave_in(0).wait_recv()
        own(5)
    with jax.named_scope("z1fin"):
        finish(11)
        own(14)
        own(15)
    with jax.named_scope("s1fin"):
        finish(10)
        own(zfar)
    with jax.named_scope("relay1"):
        relay(1)
    with jax.named_scope("y0relay"):
        relay(14)
    with jax.named_scope("relay2"):
        relay(2)
    with jax.named_scope("wave1"):
        wave_in(1).wait_recv()
        own(6)
    with jax.named_scope("y1relay"):
        relay(15)
        for core in range(2):
            wave_far(2, core).start()
    with jax.named_scope("relay3"):
        relay(3)
    with jax.named_scope("relay5"):
        relay(5)
    with jax.named_scope("zfrelay"):
        relay(zfar)
        own(znear)
        own(4)
    with jax.named_scope("y0fin"):
        finish(14)
        partner(0, 1).start()
        finish(15)
        partner(1, 1).start()
        for core in range(2):
            wave_far(3, core).start()
        for core in range(2):
            wave_far(4, core).start()
    with jax.named_scope("relay6"):
        relay(6)
    with jax.named_scope("wave2"):
        wave_in(2).wait_recv()
        own(7)
    with jax.named_scope("relay4"):
        relay(4)
    with jax.named_scope("zffin"):
        finish(zfar)
        partner(far, 0).start()
    with jax.named_scope("wave3"):
        wave_in(3).wait_recv()
        own(8)
    with jax.named_scope("relay7"):
        relay(7)
    with jax.named_scope("znrelay"):
        relay(znear)
    with jax.named_scope("wave4"):
        wave_in(4).wait_recv()
        own(9)
    with jax.named_scope("fw0"):
        finish_wave(0)
    with jax.named_scope("fromF"):
        bytes_in(rt.at[1 - c, many(2, far)], half_sem.at[far])
    with jax.named_scope("b01F"):
        blocks((0,1,), far)
    with jax.named_scope("relay8"):
        relay(8)
    with jax.named_scope("znfin"):
        finish(znear)
        partner(near, 0).start()
    with jax.named_scope("fw1"):
        finish_wave(1)
    with jax.named_scope("b2F"):
        blocks((2,), far)
    with jax.named_scope("relay9"):
        relay(9)
    with jax.named_scope("fromN"):
        bytes_in(rt.at[1 - c, many(2, near)], half_sem.at[near])
    with jax.named_scope("b01N"):
        blocks((0,1,), near)
    with jax.named_scope("fw2"):
        finish_wave(2)
    with jax.named_scope("b3F"):
        blocks((3,), far)
    with jax.named_scope("fw3"):
        finish_wave(3)
    with jax.named_scope("b4F"):
        blocks((4,), far)
    with jax.named_scope("b23N"):
        blocks((2,3,), near)
    with jax.named_scope("b4N"):
        blocks((4,), near)

    with jax.named_scope("density"):
        for k in range(NK):
            dsend[k : k + 1, :] = jnp.sum(dpart[k], axis=0, keepdims=True)
        dslot[band] = dsend[...]
        for d in range(1, 16):
            density_copy(d).start()

    with jax.named_scope("drain"):
        bytes_out(wave.at[:, pl.ds(0, 640)], out_sem.at[PARTNER_WAVE])
        bytes_out(wave.at[:, pl.ds(0, 1280)], out_sem.at[FAR_WAVE])
        bytes_out(w.at[0, 0, pl.ds(0, 480), :], out_sem.at[SCATTER])
        bytes_out(stage.at[pl.ds(0, 3)], out_sem.at[SPREAD])
        bytes_out(w.at[:, :, pl.ds(0, 1280), :], out_sem.at[RING_X])
        bytes_out(w.at[:, :, pl.ds(0, 1280), :], out_sem.at[RING_YZ])
        bytes_out(rt.at[c], out_sem.at[CORE])
        bytes_out(occ_rows.at[pl.ds(0, 3)], out_sem.at[OCC])

    with jax.named_scope("density_in"):
        bytes_in(dslot.at[pl.ds(0, 15)], in_sem.at[DENSITY])
        for g in range(4):
            total = dslot[g] + dslot[4 + g] + dslot[8 + g] + dslot[12 + g]
            dens[g * NK : (g + 1) * NK, :] = total[:NK] * (1.0 / NB)

    with jax.named_scope("out_in"):
        bytes_in(out.at[:, pl.ds(0, 1920)], in_sem.at[RESULT])
        few = out.at[:, pl.ds(0, 640)]
        pltpu.make_async_copy(few, few, in_sem.at[OWN_RESULT]).wait()
    with jax.named_scope("out_sent"):
        bytes_out(out.at[:, pl.ds(0, 1920)], out_sem.at[RESULT])
        bytes_out(dslot.at[pl.ds(0, 15)], out_sem.at[DENSITY])


def per_device(wave, ritz, occupation):
    occ = occupation.reshape(1, 256)
    dma = pltpu.SemaphoreType.DMA
    vmem = pl.BlockSpec(memory_space=pltpu.VMEM)
    anywhere = pl.BlockSpec(memory_space=pl.ANY)
    rotated, density = pl.pallas_call(
        kernel,
        out_shape=(
            jax.ShapeDtypeStruct((256, 2560), BF16),
            jax.ShapeDtypeStruct((20, 128), F32),
        ),
        in_specs=[anywhere, vmem, vmem],
        out_specs=(anywhere, vmem),
        scratch_shapes=[
            pltpu.VMEM((2, 4, 4, 16, 256), BF16),
            pltpu.VMEM((4, 4, 16, 512), BF16),
            pltpu.VMEM((2, 4, 4, 4, 16, 2048), BF16),
            pltpu.VMEM((3, 2, 2048, 256), BF16),
            pltpu.VMEM((NK, 4, 256, 128), BF16),
            pltpu.VMEM((4, 8, 256), F32),
            pltpu.VMEM((4, 256, 128), F32),
            pltpu.VMEM((NK, 8, 128), F32),
            pltpu.VMEM((8, 128), F32),
            pltpu.VMEM((16, 8, 128), F32),
            dma((11,)), dma((11,)), dma((NK,)), dma((N_RINGS, 3)), dma((6,)),
        ],
        compiler_params=pltpu.CompilerParams(
            has_side_effects=True, collective_id=0, vmem_limit_bytes=60 * 1024 * 1024
        ),
        name="rotate",
    )(wave, ritz, occ)
    return rotated, density.reshape(2560)


def solution(mesh):
    return jax.shard_map(
        per_device,
        mesh=mesh,
        in_specs=(P("band", "grid"), P("band", "grid"), P("band")),
        out_specs=(P("band", "grid"), P("grid")),
        check_vma=False,
    )
```

```python
import jax
import jax.numpy as jnp
from jax import lax
from jax.experimental import pallas as pl
from jax.experimental.pallas import tpu as pltpu
from jax.sharding import PartitionSpec as P

NB = 4096
MESH = pl.DeviceIdType.MESH
F32, BF16 = jnp.float32, jnp.bfloat16

VM = 24 * 1024 * 1024
NK = 5
CA = 1536

N_RINGS = 18

PARTNER_WAVE, FAR_WAVE, SCATTER, SPREAD, RING_X, RING_YZ, CORE, OCC, RESULT, DENSITY, LOCAL = range(11)
OWN_RESULT, RITZ, OCC_HERE = RING_X, RING_YZ, CORE


def at(x, y, z, core):
    return (x * 4 + (y // 2) * 2 + core, (y % 2) * 4 + z)


def kernel(
    wave, ritz, occ, out, dens,
    ritz_here, occ_here, rt_src, stage, rt, w, cbuf, occ_rows, occ_cols, dpart, dsend, dslot,
    out_sem, in_sem, wave_sem, ring_sem, half_sem,
):
    band, grid = lax.axis_index("band"), lax.axis_index("grid")
    x, yhi, c = band // 4, (band // 2) % 2, band % 2
    ylo, z = grid // 4, grid % 4
    y = yhi * 2 + ylo
    xj = 2 * ylo + z // 2
    zb = z % 2
    mine = yhi * 2 + c
    near, far = yhi, 1 - yhi

    def many(n, i):
        return pl.ds(pl.multiple_of(i * n, n), n)

    def send(src, dst, send_sem, recv_sem, device):
        return pltpu.make_async_remote_copy(
            src_ref=src, dst_ref=dst, send_sem=send_sem, recv_sem=recv_sem,
            device_id=device, device_id_type=MESH,
        )

    def cells(k):
        return pl.ds(k * 128, 128)

    def wave_local():
        return pltpu.make_async_copy(
            wave.at[:, many(640, yhi * 2 + c)], w.at[c, many(256, x * 2 + near)], in_sem.at[LOCAL]
        )

    def wave_partner(p):
        first, n = ((0, 128), (128, 512))[p]
        col = pl.multiple_of((yhi * 2 + 1 - c) * 640 + first, 128)
        return send(
            wave.at[:, pl.ds(col, n)], w.at[c, many(256, x * 2 + near), pl.ds(first, n)],
            out_sem.at[PARTNER_WAVE], half_sem.at[1] if p else in_sem.at[PARTNER_WAVE],
            at(x, y, z, 1 - c),
        )

    def wave_far(k, core):
        col = pl.multiple_of((1 - yhi) * 1280 + core * 640 + k * 128, 128)
        return send(
            wave.at[:, pl.ds(col, 128)],
            w.at[c, many(256, x * 2 + near), cells(k)],
            out_sem.at[FAR_WAVE], wave_sem.at[k], at(x, (y + 2) % 4, z, core),
        )

    def wave_in(k):
        rows = w.at[:, many(256, x * 2 + far), cells(k)]
        return send(rows, rows, out_sem.at[FAR_WAVE], wave_sem.at[k], at(x, (y + 2) % 4, z, c))

    def scatter(d, src):
        p = (z * 4 + y + (16 - d if src else d)) % 16
        zp, yp = p // 4, p % 4
        ys, zs = (yp, zp) if src else (y, z)
        return send(
            rt_src.at[:, zp, yp],
            stage.at[2 * (ys % 2) + zs // 2, many(2, zs % 2), :, many(256, ys // 2)],
            out_sem.at[SCATTER], in_sem.at[SCATTER], at(x, yp, zp, c),
        )

    def spread(d, src):
        other = (x + (4 - d if src else d)) % 4
        return send(
            stage.at[other], rt.at[c, :, z, y, :, many(512, other if src else x)],
            out_sem.at[SPREAD], in_sem.at[SPREAD], at(other, y, z, c),
        )

    def ring(i):
        if i < 10:
            k, rows = i % 5, (near if i < 5 else far)
            block = lambda v, h: w.at[h, many(256, v * 2 + rows), cells(k)]
        elif i == 10:
            block = lambda v, h: rt.at[c, :, z, v, :, pl.ds(h * (CA // 2), CA // 2)]
        elif i == 11:
            n = (2048 - CA) // 2
            block = lambda v, h: rt.at[c, :, v, y, :, pl.ds(CA + h * n, n)]
        elif i < 16:
            block = lambda v, h: rt.at[c, pl.ds(h * 2, 2), v, (y + i - 12) % 4, :, pl.ds(0, CA)]
        else:
            n = 2048 - CA
            block = lambda v, h: rt.at[c, pl.ds((i - 16) * 2, 2), pl.ds(h * 2, 2), v, :, pl.ds(CA, n)]
        return block

    def ring_copy(i, j, v, h):
        block, slot = ring(i), i
        axis = "x" if i < 10 else "y" if i in (10, 16, 17) else "z"
        to = 1 if j < 3 else 3
        if axis == "x":
            me, device = x, at((x + to) % 4, y, z, c)
        elif axis == "y":
            me, device = y, at(x, (y + to) % 4, z, c)
        else:
            me, device = z, at(x, y, (z + to) % 4, c)
        ref = block((me + v) % 4, h)
        sent = out_sem.at[RING_X if axis == "x" else RING_YZ]
        if j in (0, 3):
            got = ring_sem.at[slot, j // 3]
        elif axis == "x":
            got = half_sem.at[2 + max(slot % 5 - 1, 0)]
        else:
            got = ring_sem.at[slot, 3 if slot == 10 and j in (2, 5) else 2]
        return send(ref, ref, sent, got, device)

    def own_first(i):
        ring_copy(i, 0, 0, 0).start()
        ring_copy(i, 3, 0, 1).start()

    def own_rest(i):
        ring_copy(i, 1, 0, 1).start()
        ring_copy(i, 4, 0, 0).start()

    def own(i):
        own_first(i)
        own_rest(i)

    def relay(i):
        ring_copy(i, 0, 3, 0).wait_recv()
        ring_copy(i, 2, 3, 0).start()
        ring_copy(i, 3, 1, 1).wait_recv()
        ring_copy(i, 5, 1, 1).start()

    def bytes_in(ref, sem):
        send(ref, ref, out_sem.at[0], sem, at(x, y, z, 1 - c)).wait_recv()

    def bytes_out(ref, sem):
        send(ref, ref, sem, in_sem.at[0], at(x, y, z, 1 - c)).wait_send()

    def finish(i, part=0):
        low, high = pl.ds(0, CA), pl.ds(CA, 2048 - CA)
        if i == 10:
            bytes_in(rt.at[c, :, 0, 0, :, low], ring_sem.at[i, 2 + part])
        elif i == 11:
            bytes_in(rt.at[c, :, pl.ds(0, 2), 0, :, high], ring_sem.at[i, 2])
        elif i < 16:
            bytes_in(rt.at[c, :, pl.ds(0, 2), 0, :, low], ring_sem.at[i, 2])
        else:
            bytes_in(rt.at[c, pl.ds(0, 2), :, pl.ds(0, 2), :, high], ring_sem.at[i, 2])

    def finish_wave(g):
        bytes_in(rt.at[0, 0, pl.ds(0, 2 if g else 4)], half_sem.at[2 + g])

    def partner(p):
        if p < 4:
            ref = rt.at[c, :, :, (y + p) % 4, :, pl.ds(0, CA)]
        else:
            ref = rt.at[c, pl.ds((p - 4) * 2, 2), :, :, :, pl.ds(CA, 2048 - CA)]
        return send(ref, ref, out_sem.at[CORE], half_sem.at[0], at(x, y, z, 1 - c))

    def occ_copy(d, src=False):
        yy = y if d == 0 else (y + 2) % 4
        cc = c if d == 1 else 1 - c
        row = (yy // 2) * 2 + cc if src else mine
        return send(
            occ_rows.at[mine], occ_rows.at[row], out_sem.at[OCC], in_sem.at[OCC], at(x, yy, z, cc)
        )

    def result(k, hi, core):
        return send(
            cbuf.at[k, hi * 2 + core], out.at[:, many(128, yhi * 10 + c * 5 + k)],
            out_sem.at[RESULT], in_sem.at[RESULT], at(x, hi * 2 + ylo, z, core),
        )

    def result_here(k):
        return pltpu.make_async_copy(
            cbuf.at[k, mine], out.at[:, many(128, yhi * 10 + c * 5 + k)], in_sem.at[OWN_RESULT]
        )

    def density_copy(d):
        to = at((x + d // 4) % 4, (y + 2 * ((d // 2) % 2)) % 4, z, (c + d) % 2)
        return send(dsend, dslot.at[band], out_sem.at[DENSITY], in_sem.at[DENSITY], to)

    def take(k, s, summed):
        rounded = summed.astype(BF16)
        cbuf[k, s] = rounded
        values = rounded.astype(F32)
        terms = occ_cols[s] * values * values
        dpart[k] += terms.reshape(32, 8, 128).sum(axis=0)

    def product(s, ks):
        cols = pl.ds(ks[0] * 128, 128 * len(ks))
        parts = [
            jnp.dot(
                rt[v, s].reshape(256, 2048), w[v, :, cols], preferred_element_type=F32
            )
            for v in range(2)
        ]
        return parts[0] + parts[1]

    def blocks(ks, hi):
        @pl.loop(0, 2)
        def _(core):
            s = hi * 2 + core
            summed = product(s, ks)
            for n, k in enumerate(ks):
                take(k, s, summed[:, n * 128 : (n + 1) * 128])
            if hi is far:
                for k in ks:
                    result(k, hi, core).start()

        if hi is near:
            for k in ks:
                result(k, hi, 1 - c).start()
            for k in ks:
                result_here(k).start()

    with jax.named_scope("signal"):
        load_ritz = pltpu.make_async_copy(ritz, ritz_here, in_sem.at[RITZ])
        load_occ = pltpu.make_async_copy(occ, occ_here, in_sem.at[OCC_HERE])
        load_ritz.start()
        load_occ.start()
        wave_local().start()
        peers = []
        for d in range(1, 16):
            p = (z * 4 + y + d) % 16
            peers.append(at(x, p % 4, p // 4, c))
        for d in range(1, 16):
            if d != 2:
                peers.append(at((x + d // 4) % 4, (y + 2 * ((d // 2) % 2)) % 4, z, (c + d) % 2))
        barrier = pltpu.get_barrier_semaphore()
        for peer in peers:
            pl.semaphore_signal(barrier, inc=1, device_id=peer, device_id_type=MESH)

    with jax.named_scope("transpose"):
        load_ritz.wait()
        load_occ.wait()
        rt_src[...] = ritz_here[...].T.reshape(2, 4, 4, 16, 256)
        occ_rows[mine] = jnp.broadcast_to(occ_here[...], (8, 256))
        stage[xj, many(2, zb), :, many(256, yhi)] = rt_src[:, z, y]
        dpart[...] = jnp.zeros_like(dpart)
        dsend[...] = jnp.zeros_like(dsend)
    with jax.named_scope("barrier"):
        pl.semaphore_wait(barrier, len(peers))

    with jax.named_scope("start"):
        for d in range(1, 16):
            scatter(d, 0).start()
        wave_local().wait()
        for p in range(2):
            wave_partner(p).start()
        for d in range(3):
            occ_copy(d).start()
    with jax.named_scope("pw"):
        bytes_in(wave.at[:, pl.ds(0, 128)], in_sem.at[PARTNER_WAVE])
        own(0)
        bytes_in(wave.at[:, pl.ds(0, 512)], half_sem.at[1])
        own_first(1)
    with jax.named_scope("scin"):
        bytes_in(w.at[0, pl.ds(0, 192)], in_sem.at[SCATTER])
        for d in range(1, 4):
            spread(d, 0).start()
        rt[c, :, z, y, :, many(512, x)] = stage[x]
        for core in range(2):
            wave_far(0, core).start()
        for core in range(2):
            wave_far(1, core).start()
        own_rest(1)
        own(2)
        own(3)
        own(4)
    with jax.named_scope("spin"):
        bytes_in(stage.at[pl.ds(0, 3)], in_sem.at[SPREAD])
        own(10)
        own(11)
        own(12)
    with jax.named_scope("occ"):
        bytes_in(occ_rows.at[pl.ds(0, 3)], in_sem.at[OCC])
        for s in range(4):
            occ_cols[s] = jnp.broadcast_to(occ_rows[s][0:1, :], (128, 256)).T
    with jax.named_scope("s1relay"):
        relay(10)
        relay(11)
    with jax.named_scope("relay0"):
        relay(0)
    with jax.named_scope("wave0"):
        wave_in(0).wait_recv()
        own(5)
    with jax.named_scope("finA"):
        finish(10, 0)
        own(13)
        own(15)
    with jax.named_scope("z1fin"):
        finish(11)
        own(16)
        own(17)
    with jax.named_scope("p0relay"):
        relay(12)
    with jax.named_scope("s1fin"):
        finish(10, 1)
        own(14)
    with jax.named_scope("relay1"):
        relay(1)
    with jax.named_scope("y0relay"):
        relay(16)
    with jax.named_scope("relay2"):
        relay(2)
    with jax.named_scope("wave1"):
        wave_in(1).wait_recv()
        own(6)
    with jax.named_scope("y1relay"):
        relay(17)
        for core in range(2):
            wave_far(2, core).start()
    with jax.named_scope("relay3"):
        relay(3)
    with jax.named_scope("relay5"):
        relay(5)
    with jax.named_scope("p1relay"):
        relay(13)
    with jax.named_scope("p0fin"):
        finish(12)
        partner(0).start()
    with jax.named_scope("p3relay"):
        relay(15)
    with jax.named_scope("relay4"):
        relay(4)
    with jax.named_scope("y0fin"):
        finish(16)
        partner(4).start()
        finish(17)
        partner(5).start()
        for core in range(2):
            wave_far(3, core).start()
        for core in range(2):
            wave_far(4, core).start()
    with jax.named_scope("p2relay"):
        relay(14)
    with jax.named_scope("relay6"):
        relay(6)
    with jax.named_scope("wave2"):
        wave_in(2).wait_recv()
        own(7)
    with jax.named_scope("p1fin"):
        finish(13)
        partner(1).start()
    with jax.named_scope("p3fin"):
        finish(15)
        partner(3).start()
    with jax.named_scope("wave3"):
        wave_in(3).wait_recv()
        own(8)
    with jax.named_scope("relay7"):
        relay(7)
    with jax.named_scope("p2fin"):
        finish(14)
        partner(2).start()
    with jax.named_scope("wave4"):
        wave_in(4).wait_recv()
        own(9)
    with jax.named_scope("fw0"):
        finish_wave(0)
    with jax.named_scope("from"):
        bytes_in(rt.at[1 - c], half_sem.at[0])
    with jax.named_scope("b01F"):
        blocks((0,1,), far)
    with jax.named_scope("relay8"):
        relay(8)
    with jax.named_scope("b01N"):
        blocks((0,1,), near)
    with jax.named_scope("relay9"):
        relay(9)
    with jax.named_scope("fw1"):
        finish_wave(1)
    with jax.named_scope("b2F"):
        blocks((2,), far)
    with jax.named_scope("b2N"):
        blocks((2,), near)
    with jax.named_scope("fw2"):
        finish_wave(2)
    with jax.named_scope("b3F"):
        blocks((3,), far)
    with jax.named_scope("fw3"):
        finish_wave(3)
    with jax.named_scope("b4F"):
        blocks((4,), far)
    with jax.named_scope("b34N"):
        blocks((3,4,), near)

    with jax.named_scope("density"):
        for k in range(NK):
            dsend[k : k + 1, :] = jnp.sum(dpart[k], axis=0, keepdims=True)
        dslot[band] = dsend[...]
        for d in range(1, 16):
            density_copy(d).start()

    with jax.named_scope("drain"):
        bytes_out(wave.at[:, pl.ds(0, 640)], out_sem.at[PARTNER_WAVE])
        bytes_out(wave.at[:, pl.ds(0, 1280)], out_sem.at[FAR_WAVE])
        bytes_out(w.at[0, pl.ds(0, 192)], out_sem.at[SCATTER])
        bytes_out(stage.at[pl.ds(0, 3)], out_sem.at[SPREAD])
        bytes_out(w.at[:, pl.ds(0, 1536)], out_sem.at[RING_X])
        bytes_out(w.at[:, pl.ds(0, 1536)], out_sem.at[RING_YZ])
        bytes_out(rt.at[c], out_sem.at[CORE])
        bytes_out(occ_rows.at[pl.ds(0, 3)], out_sem.at[OCC])

    with jax.named_scope("density_in"):
        bytes_in(dslot.at[pl.ds(0, 15)], in_sem.at[DENSITY])
        for g in range(4):
            total = dslot[g] + dslot[4 + g] + dslot[8 + g] + dslot[12 + g]
            dens[g * NK : (g + 1) * NK, :] = total[:NK] * (1.0 / NB)

    with jax.named_scope("out_in"):
        bytes_in(out.at[:, pl.ds(0, 1920)], in_sem.at[RESULT])
        few = out.at[:, pl.ds(0, 640)]
        pltpu.make_async_copy(few, few, in_sem.at[OWN_RESULT]).wait()
    with jax.named_scope("out_sent"):
        bytes_out(out.at[:, pl.ds(0, 1920)], out_sem.at[RESULT])
        bytes_out(dslot.at[pl.ds(0, 15)], out_sem.at[DENSITY])


def per_device(wave, ritz, occupation):
    wave, ritz, occ = (
        pltpu.with_memory_space_constraint(a, pltpu.HBM)
        for a in (wave, ritz, occupation.reshape(1, 256))
    )
    dma = pltpu.SemaphoreType.DMA
    vmem = pl.BlockSpec(memory_space=pltpu.VMEM)
    anywhere = pl.BlockSpec(memory_space=pl.ANY)
    rotated, density = pl.pallas_call(
        kernel,
        out_shape=(
            jax.ShapeDtypeStruct((256, 2560), BF16),
            jax.ShapeDtypeStruct((20, 128), F32),
        ),
        in_specs=[pl.BlockSpec(memory_space=pltpu.HBM)] * 3,
        out_specs=(anywhere, vmem),
        scratch_shapes=[
            pltpu.VMEM((256, 512), BF16),
            pltpu.VMEM((1, 256), F32),
            pltpu.VMEM((2, 4, 4, 16, 256), BF16),
            pltpu.VMEM((4, 4, 16, 512), BF16),
            pltpu.VMEM((2, 4, 4, 4, 16, 2048), BF16),
            pltpu.VMEM((2, 2048, 640), BF16),
            pltpu.VMEM((NK, 4, 256, 128), BF16),
            pltpu.VMEM((4, 8, 256), F32),
            pltpu.VMEM((4, 256, 128), F32),
            pltpu.VMEM((NK, 8, 128), F32),
            pltpu.VMEM((8, 128), F32),
            pltpu.VMEM((16, 8, 128), F32),
            dma((11,)), dma((11,)), dma((NK,)), dma((N_RINGS, 4)), dma((6,)),
        ],
        compiler_params=pltpu.CompilerParams(
            has_side_effects=True, collective_id=0, vmem_limit_bytes=VM
        ),
        name="rotate",
    )(wave, ritz, occ)
    return rotated, density.reshape(2560)


def solution(mesh):
    return jax.shard_map(
        per_device,
        mesh=mesh,
        in_specs=(P("band", "grid"), P("band", "grid"), P("band")),
        out_specs=(P("band", "grid"), P("grid")),
        check_vma=False,
    )
```

```python
import jax
import jax.numpy as jnp
from jax import lax
from jax.experimental import pallas as pl
from jax.experimental.pallas import tpu as pltpu
from jax.sharding import PartitionSpec as P

NB = 4096
MESH = pl.DeviceIdType.MESH
F32, BF16 = jnp.float32, jnp.bfloat16

VM = 24 * 1024 * 1024
NK = 5
CA = 1408

N_RINGS = 18

PARTNER_WAVE, FAR_WAVE, SCATTER, SPREAD, RING_X, RING_YZ, CORE, OCC, RESULT, DENSITY, LOCAL = range(11)
OWN_RESULT, RITZ, OCC_HERE = RING_X, RING_YZ, CORE

IN_PLANE = sorted(
    ((dy, dz) for dy in range(4) for dz in range(4) if dy or dz),
    key=lambda d: -min(d[0], 4 - d[0]) - min(d[1], 4 - d[1]),
)


def at(x, y, z, core):
    return (x * 4 + (y // 2) * 2 + core, (y % 2) * 4 + z)


def kernel(
    wave, ritz, occ, out, dens,
    ritz_here, occ_here, rt_src, stage, rt, w, cbuf, occ_rows, occ_cols, dpart, dsend, dslot,
    out_sem, in_sem, wave_sem, ring_sem, half_sem,
):
    band, grid = lax.axis_index("band"), lax.axis_index("grid")
    x, yhi, c = band // 4, (band // 2) % 2, band % 2
    ylo, z = grid // 4, grid % 4
    y = yhi * 2 + ylo
    xj = 2 * ylo + z // 2
    zb = z % 2
    mine = yhi * 2 + c
    near, far = yhi, 1 - yhi

    def many(n, i):
        return pl.ds(pl.multiple_of(i * n, n), n)

    def send(src, dst, send_sem, recv_sem, device):
        return pltpu.make_async_remote_copy(
            src_ref=src, dst_ref=dst, send_sem=send_sem, recv_sem=recv_sem,
            device_id=device, device_id_type=MESH,
        )

    def cells(k):
        return pl.ds(k * 128, 128)

    def wave_local():
        return pltpu.make_async_copy(
            wave.at[:, many(640, yhi * 2 + c)], w.at[c, many(256, x * 2 + near)], in_sem.at[LOCAL]
        )

    def wave_partner(p):
        first, n = ((0, 128), (128, 512))[p]
        col = pl.multiple_of((yhi * 2 + 1 - c) * 640 + first, 128)
        return send(
            wave.at[:, pl.ds(col, n)], w.at[c, many(256, x * 2 + near), pl.ds(first, n)],
            out_sem.at[PARTNER_WAVE], half_sem.at[1] if p else in_sem.at[PARTNER_WAVE],
            at(x, y, z, 1 - c),
        )

    def wave_far(k, core):
        col = pl.multiple_of((1 - yhi) * 1280 + core * 640 + k * 128, 128)
        return send(
            wave.at[:, pl.ds(col, 128)],
            w.at[c, many(256, x * 2 + near), cells(k)],
            out_sem.at[FAR_WAVE], wave_sem.at[k], at(x, (y + 2) % 4, z, core),
        )

    def wave_in(k):
        rows = w.at[:, many(256, x * 2 + far), cells(k)]
        return send(rows, rows, out_sem.at[FAR_WAVE], wave_sem.at[k], at(x, (y + 2) % 4, z, c))

    def scatter(dy, dz):
        yp, zp = (y + dy) % 4, (z + dz) % 4
        return send(
            rt_src.at[:, zp, yp],
            stage.at[xj, many(2, zb), :, many(256, yhi)],
            out_sem.at[SCATTER], in_sem.at[SCATTER], at(x, yp, zp, c),
        )

    def spread(d):
        other = (x + d) % 4
        return send(
            stage.at[other], rt.at[c, :, z, y, :, many(512, x)],
            out_sem.at[SPREAD], in_sem.at[SPREAD], at(other, y, z, c),
        )

    def ring(i):
        if i < 10:
            k, rows = i % 5, (near if i < 5 else far)
            block = lambda v, h: w.at[h, many(256, v * 2 + rows), cells(k)]
        elif i == 10:
            block = lambda v, h: rt.at[c, pl.ds(h * 2, 2), z, v, :, pl.ds(0, CA)]
        elif i == 11:
            block = lambda v, h: rt.at[c, pl.ds(h * 2, 2), v, y, :, pl.ds(CA, 2048 - CA)]
        elif i < 16:
            block = lambda v, h: rt.at[c, pl.ds(h * 2, 2), v, (y + i - 12) % 4, :, pl.ds(0, CA)]
        else:
            n = 2048 - CA
            block = lambda v, h: rt.at[c, pl.ds((i - 16) * 2, 2), pl.ds(h * 2, 2), v, :, pl.ds(CA, n)]
        return block

    def sem_of(i, n):
        if n == 3:
            return 44 + (i == 14)
        return i * 2 + n if i < 10 else 20 + (i - 10) * 3 + n

    def ring_copy(i, j, v, h):
        block, slot = ring(i), i
        axis = "x" if i < 10 else "y" if i in (10, 16, 17) else "z"
        to = 1 if j < 3 else 3
        if axis == "x":
            me, device = x, at((x + to) % 4, y, z, c)
        elif axis == "y":
            me, device = y, at(x, (y + to) % 4, z, c)
        else:
            me, device = z, at(x, y, (z + to) % 4, c)
        ref = block((me + v) % 4, h)
        sent = out_sem.at[RING_X if axis == "x" else RING_YZ]
        if j in (0, 3):
            got = ring_sem.at[sem_of(slot, j // 3)]
        elif axis == "x":
            got = half_sem.at[2 + max(slot % 5 - 1, 0)]
        else:
            got = ring_sem.at[sem_of(slot, 3 if slot in (10, 14) and j in (2, 5) else 2)]
        return send(ref, ref, sent, got, device)

    def own_first(i):
        ring_copy(i, 0, 0, 0).start()
        ring_copy(i, 3, 0, 1).start()

    def own_rest(i):
        ring_copy(i, 1, 0, 1).start()
        ring_copy(i, 4, 0, 0).start()

    def own(i):
        own_first(i)
        own_rest(i)

    def relay(i):
        ring_copy(i, 0, 3, 0).wait_recv()
        ring_copy(i, 2, 3, 0).start()
        ring_copy(i, 3, 1, 1).wait_recv()
        ring_copy(i, 5, 1, 1).start()

    def bytes_in(ref, sem):
        send(ref, ref, out_sem.at[0], sem, at(x, y, z, 1 - c)).wait_recv()

    def bytes_out(ref, sem):
        send(ref, ref, sem, in_sem.at[0], at(x, y, z, 1 - c)).wait_send()

    def finish(i, part=0):
        low, high = pl.ds(0, CA), pl.ds(CA, 2048 - CA)
        if i in (10, 14):
            bytes_in(rt.at[c, :, 0, 0, :, low], ring_sem.at[sem_of(i, 2 + part)])
        elif i == 11:
            bytes_in(rt.at[c, :, pl.ds(0, 2), 0, :, high], ring_sem.at[sem_of(i, 2)])
        elif i < 16:
            bytes_in(rt.at[c, :, pl.ds(0, 2), 0, :, low], ring_sem.at[sem_of(i, 2)])
        else:
            bytes_in(rt.at[c, pl.ds(0, 2), :, pl.ds(0, 2), :, high], ring_sem.at[sem_of(i, 2)])

    def finish_wave(g):
        bytes_in(rt.at[0, 0, pl.ds(0, 2 if g else 4)], half_sem.at[2 + g])

    def partner(p, vs=()):
        if p == 2:
            refs = [rt.at[c, :, (z + v) % 4, (y + 2) % 4, :, pl.ds(0, CA)] for v in vs]
        elif p < 4:
            refs = [rt.at[c, :, :, (y + p) % 4, :, pl.ds(0, CA)]]
        elif p == 4:
            refs = [rt.at[c, :, :, y, :, pl.ds(CA, 2048 - CA)]]
        else:
            refs = [
                rt.at[c, pl.ds((p - 5) * 2, 2), :, (y + d) % 4, :, pl.ds(CA, 2048 - CA)]
                for d in range(1, 4)
            ]
        for ref in refs:
            send(ref, ref, out_sem.at[CORE], half_sem.at[0], at(x, y, z, 1 - c)).start()

    def occ_copy(d, src=False):
        yy = y if d == 0 else (y + 2) % 4
        cc = c if d == 1 else 1 - c
        row = (yy // 2) * 2 + cc if src else mine
        return send(
            occ_rows.at[mine], occ_rows.at[row], out_sem.at[OCC], in_sem.at[OCC], at(x, yy, z, cc)
        )

    def result(k, hi, core):
        return send(
            cbuf.at[k, hi * 2 + core], out.at[:, many(128, yhi * 10 + c * 5 + k)],
            out_sem.at[RESULT], in_sem.at[RESULT], at(x, hi * 2 + ylo, z, core),
        )

    def result_here(k):
        return pltpu.make_async_copy(
            cbuf.at[k, mine], out.at[:, many(128, yhi * 10 + c * 5 + k)], in_sem.at[OWN_RESULT]
        )

    def density_copy(d):
        to = at((x + d // 4) % 4, (y + 2 * ((d // 2) % 2)) % 4, z, (c + d) % 2)
        return send(dsend, dslot.at[band], out_sem.at[DENSITY], in_sem.at[DENSITY], to)

    def take(k, s, summed):
        rounded = summed.astype(BF16)
        cbuf[k, s] = rounded
        values = rounded.astype(F32)
        terms = occ_cols[s] * values * values
        dpart[k] += terms.reshape(32, 8, 128).sum(axis=0)

    def product(s, ks):
        cols = pl.ds(ks[0] * 128, 128 * len(ks))
        parts = [
            jnp.dot(
                rt[v, s].reshape(256, 2048), w[v, :, cols], preferred_element_type=F32
            )
            for v in range(2)
        ]
        return parts[0] + parts[1]

    def blocks(ks, hi):
        @pl.loop(0, 2)
        def _(core):
            s = hi * 2 + core
            summed = product(s, ks)
            for n, k in enumerate(ks):
                take(k, s, summed[:, n * 128 : (n + 1) * 128])
            if hi is far:
                for k in ks:
                    result(k, hi, core).start()

        if hi is near:
            for k in ks:
                result(k, hi, 1 - c).start()
            for k in ks:
                result_here(k).start()

    with jax.named_scope("signal"):
        load_ritz = pltpu.make_async_copy(ritz, ritz_here, in_sem.at[RITZ])
        load_occ = pltpu.make_async_copy(occ, occ_here, in_sem.at[OCC_HERE])
        load_ritz.start()
        load_occ.start()
        wave_local().start()
        peers = []
        for dy, dz in IN_PLANE:
            peers.append(at(x, (y + dy) % 4, (z + dz) % 4, c))
        for d in range(1, 16):
            if d != 2:
                peers.append(at((x + d // 4) % 4, (y + 2 * ((d // 2) % 2)) % 4, z, (c + d) % 2))
        barrier = pltpu.get_barrier_semaphore()
        for peer in peers:
            pl.semaphore_signal(barrier, inc=1, device_id=peer, device_id_type=MESH)

    with jax.named_scope("transpose"):
        load_ritz.wait()
        load_occ.wait()
        rt_src[...] = ritz_here[...].T.reshape(2, 4, 4, 16, 256)
        occ_rows[mine] = jnp.broadcast_to(occ_here[...], (8, 256))
        stage[xj, many(2, zb), :, many(256, yhi)] = rt_src[:, z, y]
        dpart[...] = jnp.zeros_like(dpart)
        dsend[...] = jnp.zeros_like(dsend)
    with jax.named_scope("barrier"):
        pl.semaphore_wait(barrier, len(peers))

    with jax.named_scope("start"):
        for dy, dz in IN_PLANE:
            scatter(dy, dz).start()
        wave_local().wait()
        for p in range(2):
            wave_partner(p).start()
        for d in range(3):
            occ_copy(d).start()
    with jax.named_scope("pw"):
        bytes_in(wave.at[:, pl.ds(0, 128)], in_sem.at[PARTNER_WAVE])
        own(0)
        bytes_in(wave.at[:, pl.ds(0, 512)], half_sem.at[1])
        own_first(1)
    with jax.named_scope("scin"):
        bytes_in(w.at[0, pl.ds(0, 192)], in_sem.at[SCATTER])
        for d in (2, 1, 3):
            spread(d).start()
        rt[c, :, z, y, :, many(512, x)] = stage[x]
        for core in range(2):
            wave_far(0, core).start()
        for core in range(2):
            wave_far(1, core).start()
        own_rest(1)
        own(2)
        own(3)
        own(4)
    with jax.named_scope("spin"):
        bytes_in(stage.at[pl.ds(0, 3)], in_sem.at[SPREAD])
        own(10)
        own(11)
        own(12)
    with jax.named_scope("occ"):
        bytes_in(occ_rows.at[pl.ds(0, 3)], in_sem.at[OCC])
        for s in range(4):
            occ_cols[s] = jnp.broadcast_to(occ_rows[s][0:1, :], (128, 256)).T
    with jax.named_scope("s1relay"):
        relay(10)
        relay(11)
        for core in range(2):
            wave_far(2, core).start()
    with jax.named_scope("relay0"):
        relay(0)
    with jax.named_scope("wave0"):
        wave_in(0).wait_recv()
        own(5)
    with jax.named_scope("finA"):
        finish(10, 0)
        own(13)
        own(15)
    with jax.named_scope("z1fin"):
        finish(11)
        own(16)
        own(17)
        partner(4)
    with jax.named_scope("p0relay"):
        relay(12)
    with jax.named_scope("s1fin"):
        finish(10, 1)
        own(14)
        partner(2, (0,))
    with jax.named_scope("relay1"):
        relay(1)
    with jax.named_scope("y0relay"):
        relay(16)
    with jax.named_scope("relay2"):
        relay(2)
    with jax.named_scope("wave1"):
        wave_in(1).wait_recv()
        own(6)
    with jax.named_scope("y1relay"):
        relay(17)
        for core in range(2):
            wave_far(3, core).start()
        for core in range(2):
            wave_far(4, core).start()
    with jax.named_scope("relay3"):
        relay(3)
    with jax.named_scope("relay5"):
        relay(5)
    with jax.named_scope("p1relay"):
        relay(13)
    with jax.named_scope("p0fin"):
        finish(12)
        partner(0)
    with jax.named_scope("y0fin"):
        finish(16)
        partner(5)
    with jax.named_scope("p3relay"):
        relay(15)
    with jax.named_scope("relay4"):
        relay(4)
    with jax.named_scope("p2relay"):
        relay(14)
    with jax.named_scope("relay6"):
        relay(6)
    with jax.named_scope("wave2"):
        wave_in(2).wait_recv()
        own(7)
    with jax.named_scope("p1fin"):
        finish(13)
        partner(1)
    with jax.named_scope("y1fin"):
        finish(17)
        partner(6)
    with jax.named_scope("p3fin"):
        finish(15)
        partner(3)
    with jax.named_scope("wave3"):
        wave_in(3).wait_recv()
        own(8)
    with jax.named_scope("p2fin"):
        finish(14, 0)
        partner(2, (1,3))
        finish(14, 1)
        partner(2, (2,))
    with jax.named_scope("relay7"):
        relay(7)
    with jax.named_scope("fw0"):
        finish_wave(0)
    with jax.named_scope("wave4"):
        wave_in(4).wait_recv()
        own(9)
    with jax.named_scope("from"):
        bytes_in(rt.at[1 - c], half_sem.at[0])
    with jax.named_scope("b01F"):
        blocks((0,1,), far)
    with jax.named_scope("relay8"):
        relay(8)
    with jax.named_scope("b01N"):
        blocks((0,1,), near)
    with jax.named_scope("relay9"):
        relay(9)
    with jax.named_scope("fw1"):
        finish_wave(1)
    with jax.named_scope("b2F"):
        blocks((2,), far)
    with jax.named_scope("b2N"):
        blocks((2,), near)
    with jax.named_scope("fw2"):
        finish_wave(2)
    with jax.named_scope("b3F"):
        blocks((3,), far)
    with jax.named_scope("fw3"):
        finish_wave(3)
    with jax.named_scope("b4F"):
        blocks((4,), far)
    with jax.named_scope("b34N"):
        blocks((3,4,), near)

    with jax.named_scope("density"):
        for k in range(NK):
            dsend[k : k + 1, :] = jnp.sum(dpart[k], axis=0, keepdims=True)
        dslot[band] = dsend[...]
        for d in range(1, 16):
            density_copy(d).start()

    with jax.named_scope("drain"):
        bytes_out(wave.at[:, pl.ds(0, 640)], out_sem.at[PARTNER_WAVE])
        bytes_out(wave.at[:, pl.ds(0, 1280)], out_sem.at[FAR_WAVE])
        bytes_out(w.at[0, pl.ds(0, 192)], out_sem.at[SCATTER])
        bytes_out(stage.at[pl.ds(0, 3)], out_sem.at[SPREAD])
        bytes_out(w.at[:, pl.ds(0, 1536)], out_sem.at[RING_X])
        bytes_out(w.at[:, pl.ds(0, 1536)], out_sem.at[RING_YZ])
        bytes_out(rt.at[c], out_sem.at[CORE])
        bytes_out(occ_rows.at[pl.ds(0, 3)], out_sem.at[OCC])

    with jax.named_scope("density_in"):
        bytes_in(dslot.at[pl.ds(0, 15)], in_sem.at[DENSITY])
        for g in range(4):
            total = dslot[g] + dslot[4 + g] + dslot[8 + g] + dslot[12 + g]
            dens[g * NK : (g + 1) * NK, :] = total[:NK] * (1.0 / NB)

    with jax.named_scope("out_in"):
        bytes_in(out.at[:, pl.ds(0, 1920)], in_sem.at[RESULT])
        few = out.at[:, pl.ds(0, 640)]
        pltpu.make_async_copy(few, few, in_sem.at[OWN_RESULT]).wait()
    with jax.named_scope("out_sent"):
        bytes_out(out.at[:, pl.ds(0, 1920)], out_sem.at[RESULT])
        bytes_out(dslot.at[pl.ds(0, 15)], out_sem.at[DENSITY])


def per_device(wave, ritz, occupation):
    wave, ritz, occ = (
        pltpu.with_memory_space_constraint(a, pltpu.HBM)
        for a in (wave, ritz, occupation.reshape(1, 256))
    )
    dma = pltpu.SemaphoreType.DMA
    vmem = pl.BlockSpec(memory_space=pltpu.VMEM)
    anywhere = pl.BlockSpec(memory_space=pl.ANY)
    rotated, density = pl.pallas_call(
        kernel,
        out_shape=(
            jax.ShapeDtypeStruct((256, 2560), BF16),
            jax.ShapeDtypeStruct((20, 128), F32),
        ),
        in_specs=[pl.BlockSpec(memory_space=pltpu.HBM)] * 3,
        out_specs=(anywhere, vmem),
        scratch_shapes=[
            pltpu.VMEM((256, 512), BF16),
            pltpu.VMEM((1, 256), F32),
            pltpu.VMEM((2, 4, 4, 16, 256), BF16),
            pltpu.VMEM((4, 4, 16, 512), BF16),
            pltpu.VMEM((2, 4, 4, 4, 16, 2048), BF16),
            pltpu.VMEM((2, 2048, 640), BF16),
            pltpu.VMEM((NK, 4, 256, 128), BF16),
            pltpu.VMEM((4, 8, 256), F32),
            pltpu.VMEM((4, 256, 128), F32),
            pltpu.VMEM((NK, 8, 128), F32),
            pltpu.VMEM((8, 128), F32),
            pltpu.VMEM((16, 8, 128), F32),
            dma((11,)), dma((11,)), dma((NK,)), dma((46,)), dma((6,)),
        ],
        compiler_params=pltpu.CompilerParams(
            has_side_effects=True, collective_id=0, vmem_limit_bytes=VM
        ),
        name="rotate",
    )(wave, ritz, occ)
    return rotated, density.reshape(2560)


def solution(mesh):
    return jax.shard_map(
        per_device,
        mesh=mesh,
        in_specs=(P("band", "grid"), P("band", "grid"), P("band")),
        out_specs=(P("band", "grid"), P("grid")),
        check_vma=False,
    )
```

```python
import jax
import jax.numpy as jnp
from jax import lax
from jax.experimental import pallas as pl
from jax.experimental.pallas import tpu as pltpu
from jax.sharding import PartitionSpec as P

NB = 4096
MESH = pl.DeviceIdType.MESH
F32, BF16 = jnp.float32, jnp.bfloat16

VM = 24 * 1024 * 1024
NK = 5
CA = 1408

N_RINGS = 18

PARTNER_WAVE, FAR_WAVE, SCATTER, SPREAD, RING_X, RING_YZ, CORE, OCC, RESULT, DENSITY, LOCAL = range(11)
OWN_RESULT, RITZ, OCC_HERE = RING_X, RING_YZ, CORE

def hops(*steps):
    return sum(min(step, 4 - step) for step in steps)


IN_PLANE = sorted(
    ((hops(dy, dz), dy, dz) for dy in range(4) for dz in range(4) if dy or dz),
    key=lambda d: -d[0],
)
SHARERS = [
    (hops(dx, dy), dx, dy, dc)
    for dx in range(4) for dy in (0, 2) for dc in range(2)
    if (dx, dy, dc) not in ((0, 0, 0), (0, 2, 0))
]


def at(x, y, z, core):
    return (x * 4 + (y // 2) * 2 + core, (y % 2) * 4 + z)


def kernel(
    wave, ritz, occ, out, dens,
    ritz_here, occ_here, rt_src, stage, rt, w, cbuf, occ_rows, occ_cols, dpart, dsend, dslot,
    out_sem, in_sem, wave_sem, ring_sem, half_sem,
):
    band, grid = lax.axis_index("band"), lax.axis_index("grid")
    x, yhi, c = band // 4, (band // 2) % 2, band % 2
    ylo, z = grid // 4, grid % 4
    y = yhi * 2 + ylo
    xj = 2 * ylo + z // 2
    zb = z % 2
    mine = yhi * 2 + c
    near, far = yhi, 1 - yhi

    def many(n, i):
        return pl.ds(pl.multiple_of(i * n, n), n)

    def send(src, dst, send_sem, recv_sem, device):
        return pltpu.make_async_remote_copy(
            src_ref=src, dst_ref=dst, send_sem=send_sem, recv_sem=recv_sem,
            device_id=device, device_id_type=MESH,
        )

    def cells(k):
        return pl.ds(k * 128, 128)

    def wave_local():
        return pltpu.make_async_copy(
            wave.at[:, many(640, yhi * 2 + c)], w.at[c, many(256, x * 2 + near)], in_sem.at[LOCAL]
        )

    def wave_partner(p):
        first, n = ((0, 128), (128, 512))[p]
        col = pl.multiple_of((yhi * 2 + 1 - c) * 640 + first, 128)
        return send(
            wave.at[:, pl.ds(col, n)], w.at[c, many(256, x * 2 + near), pl.ds(first, n)],
            out_sem.at[PARTNER_WAVE], half_sem.at[1] if p else in_sem.at[PARTNER_WAVE],
            at(x, y, z, 1 - c),
        )

    def wave_far(k, core):
        col = pl.multiple_of((1 - yhi) * 1280 + core * 640 + k * 128, 128)
        return send(
            wave.at[:, pl.ds(col, 128)],
            w.at[c, many(256, x * 2 + near), cells(k)],
            out_sem.at[FAR_WAVE], wave_sem.at[k], at(x, (y + 2) % 4, z, core),
        )

    def wave_in(k):
        rows = w.at[:, many(256, x * 2 + far), cells(k)]
        return send(rows, rows, out_sem.at[FAR_WAVE], wave_sem.at[k], at(x, (y + 2) % 4, z, c))

    def scatter(dy, dz):
        yp, zp = (y + dy) % 4, (z + dz) % 4
        return send(
            rt_src.at[:, zp, yp],
            stage.at[xj, many(2, zb), :, many(256, yhi)],
            out_sem.at[SCATTER], in_sem.at[SCATTER], at(x, yp, zp, c),
        )

    def spread(d):
        other = (x + d) % 4
        return send(
            stage.at[other], rt.at[c, :, z, y, :, many(512, x)],
            out_sem.at[SPREAD], in_sem.at[SPREAD], at(other, y, z, c),
        )

    def ring(i):
        if i < 10:
            k, rows = i % 5, (near if i < 5 else far)
            block = lambda v, h: w.at[h, many(256, v * 2 + rows), cells(k)]
        elif i == 10:
            block = lambda v, h: rt.at[c, pl.ds(h * 2, 2), z, v, :, pl.ds(0, CA)]
        elif i == 11:
            block = lambda v, h: rt.at[c, pl.ds(h * 2, 2), v, y, :, pl.ds(CA, 2048 - CA)]
        elif i < 16:
            block = lambda v, h: rt.at[c, pl.ds(h * 2, 2), v, (y + i - 12) % 4, :, pl.ds(0, CA)]
        else:
            n = 2048 - CA
            block = lambda v, h: rt.at[c, pl.ds((i - 16) * 2, 2), pl.ds(h * 2, 2), v, :, pl.ds(CA, n)]
        return block

    def sem_of(i, n):
        if n == 3:
            return 44 + (i == 14)
        return i * 2 + n if i < 10 else 20 + (i - 10) * 3 + n

    def ring_copy(i, j, v, h):
        block, slot = ring(i), i
        axis = "x" if i < 10 else "y" if i in (10, 16, 17) else "z"
        to = 1 if j < 3 else 3
        if axis == "x":
            me, device = x, at((x + to) % 4, y, z, c)
        elif axis == "y":
            me, device = y, at(x, (y + to) % 4, z, c)
        else:
            me, device = z, at(x, y, (z + to) % 4, c)
        ref = block((me + v) % 4, h)
        sent = out_sem.at[RING_X if axis == "x" else RING_YZ]
        if j in (0, 3):
            got = ring_sem.at[sem_of(slot, j // 3)]
        elif axis == "x":
            got = half_sem.at[2 + max(slot % 5 - 1, 0)]
        else:
            got = ring_sem.at[sem_of(slot, 3 if slot in (10, 14) and j in (2, 5) else 2)]
        return send(ref, ref, sent, got, device)

    def own_first(i):
        ring_copy(i, 0, 0, 0).start()
        ring_copy(i, 3, 0, 1).start()

    def own_rest(i):
        ring_copy(i, 1, 0, 1).start()
        ring_copy(i, 4, 0, 0).start()

    def own(i):
        own_first(i)
        own_rest(i)

    def relay(i):
        ring_copy(i, 0, 3, 0).wait_recv()
        ring_copy(i, 2, 3, 0).start()
        ring_copy(i, 3, 1, 1).wait_recv()
        ring_copy(i, 5, 1, 1).start()

    def bytes_in(ref, sem):
        send(ref, ref, out_sem.at[0], sem, at(x, y, z, 1 - c)).wait_recv()

    def bytes_out(ref, sem):
        send(ref, ref, sem, in_sem.at[0], at(x, y, z, 1 - c)).wait_send()

    def finish(i, part=0):
        low, high = pl.ds(0, CA), pl.ds(CA, 2048 - CA)
        if i in (10, 14):
            bytes_in(rt.at[c, :, 0, 0, :, low], ring_sem.at[sem_of(i, 2 + part)])
        elif i == 11:
            bytes_in(rt.at[c, :, pl.ds(0, 2), 0, :, high], ring_sem.at[sem_of(i, 2)])
        elif i < 16:
            bytes_in(rt.at[c, :, pl.ds(0, 2), 0, :, low], ring_sem.at[sem_of(i, 2)])
        else:
            bytes_in(rt.at[c, pl.ds(0, 2), :, pl.ds(0, 2), :, high], ring_sem.at[sem_of(i, 2)])

    def finish_wave(g):
        bytes_in(rt.at[0, 0, pl.ds(0, 2 if g else 4)], half_sem.at[2 + g])

    def partner(p, vs=()):
        if p == 2:
            refs = [rt.at[c, :, (z + v) % 4, (y + 2) % 4, :, pl.ds(0, CA)] for v in vs]
        elif p < 4:
            refs = [rt.at[c, :, :, (y + p) % 4, :, pl.ds(0, CA)]]
        elif p == 4:
            refs = [rt.at[c, :, :, y, :, pl.ds(CA, 2048 - CA)]]
        else:
            refs = [
                rt.at[c, pl.ds((p - 5) * 2, 2), :, (y + d) % 4, :, pl.ds(CA, 2048 - CA)]
                for d in range(1, 4)
            ]
        for ref in refs:
            send(ref, ref, out_sem.at[CORE], half_sem.at[0], at(x, y, z, 1 - c)).start()

    def occ_copy(d, src=False):
        yy = y if d == 0 else (y + 2) % 4
        cc = c if d == 1 else 1 - c
        row = (yy // 2) * 2 + cc if src else mine
        return send(
            occ_rows.at[mine], occ_rows.at[row], out_sem.at[OCC], in_sem.at[OCC], at(x, yy, z, cc)
        )

    def result(k, hi, core):
        return send(
            cbuf.at[k, hi * 2 + core], out.at[:, many(128, yhi * 10 + c * 5 + k)],
            out_sem.at[RESULT], in_sem.at[RESULT], at(x, hi * 2 + ylo, z, core),
        )

    def result_here(k):
        return pltpu.make_async_copy(
            cbuf.at[k, mine], out.at[:, many(128, yhi * 10 + c * 5 + k)], in_sem.at[OWN_RESULT]
        )

    def density_copy(d):
        to = at((x + d // 4) % 4, (y + 2 * ((d // 2) % 2)) % 4, z, (c + d) % 2)
        return send(dsend, dslot.at[band], out_sem.at[DENSITY], in_sem.at[DENSITY], to)

    def take(k, s, summed):
        rounded = summed.astype(BF16)
        cbuf[k, s] = rounded
        values = rounded.astype(F32)
        terms = occ_cols[s] * values * values
        dpart[k] += terms.reshape(32, 8, 128).sum(axis=0)

    def product(s, ks):
        cols = pl.ds(ks[0] * 128, 128 * len(ks))
        parts = [
            jnp.dot(
                rt[v, s].reshape(256, 2048), w[v, :, cols], preferred_element_type=F32
            )
            for v in range(2)
        ]
        return parts[0] + parts[1]

    def blocks(ks, hi):
        @pl.loop(0, 2)
        def _(core):
            s = hi * 2 + core
            summed = product(s, ks)
            for n, k in enumerate(ks):
                take(k, s, summed[:, n * 128 : (n + 1) * 128])
            if hi is far:
                for k in ks:
                    result(k, hi, core).start()

        if hi is near:
            for k in ks:
                result(k, hi, 1 - c).start()
            for k in ks:
                result_here(k).start()

    with jax.named_scope("signal"):
        peers = [(n, at((x + dx) % 4, (y + dy) % 4, z, (c + dc) % 2)) for n, dx, dy, dc in SHARERS]
        peers += [(n, at(x, (y + dy) % 4, (z + dz) % 4, c)) for n, dy, dz in IN_PLANE]
        peers = [peer for _, peer in sorted(peers, key=lambda p: -p[0])]
        barrier = pltpu.get_barrier_semaphore()
        for peer in peers:
            pl.semaphore_signal(barrier, inc=1, device_id=peer, device_id_type=MESH)
        load_ritz = pltpu.make_async_copy(ritz, ritz_here, in_sem.at[RITZ])
        load_occ = pltpu.make_async_copy(occ, occ_here, in_sem.at[OCC_HERE])
        load_ritz.start()
        load_occ.start()
        wave_local().start()

    with jax.named_scope("transpose"):
        load_ritz.wait()
        load_occ.wait()
        rt_src[...] = ritz_here[...].T.reshape(2, 4, 4, 16, 256)
        occ_rows[mine] = jnp.broadcast_to(occ_here[...], (8, 256))
        stage[xj, many(2, zb), :, many(256, yhi)] = rt_src[:, z, y]
        dpart[...] = jnp.zeros_like(dpart)
        dsend[...] = jnp.zeros_like(dsend)
    with jax.named_scope("barrier"):
        pl.semaphore_wait(barrier, len(peers))

    with jax.named_scope("start"):
        for _, dy, dz in IN_PLANE:
            scatter(dy, dz).start()
        wave_local().wait()
        for p in range(2):
            wave_partner(p).start()
        for d in range(3):
            occ_copy(d).start()
    with jax.named_scope("pw"):
        bytes_in(wave.at[:, pl.ds(0, 128)], in_sem.at[PARTNER_WAVE])
        own(0)
        bytes_in(wave.at[:, pl.ds(0, 512)], half_sem.at[1])
    with jax.named_scope("scin"):
        bytes_in(w.at[0, pl.ds(0, 192)], in_sem.at[SCATTER])
        for d in (2, 1, 3):
            spread(d).start()
        rt[c, :, z, y, :, many(512, x)] = stage[x]
        for core in range(2):
            wave_far(0, core).start()
        for core in range(2):
            wave_far(1, core).start()
        own(1)
        own(2)
        own(3)
        own(4)
    with jax.named_scope("spin"):
        bytes_in(stage.at[pl.ds(0, 3)], in_sem.at[SPREAD])
        own(11)
        own(12)
        own(10)
    with jax.named_scope("occ"):
        bytes_in(occ_rows.at[pl.ds(0, 3)], in_sem.at[OCC])
        for s in range(4):
            occ_cols[s] = jnp.broadcast_to(occ_rows[s][0:1, :], (128, 256)).T
    with jax.named_scope("s1relay"):
        relay(10)
        relay(11)
        for core in range(2):
            wave_far(2, core).start()
    with jax.named_scope("relay0"):
        relay(0)
    with jax.named_scope("wave0"):
        wave_in(0).wait_recv()
        own(5)
    with jax.named_scope("finA"):
        finish(10, 0)
        own(13)
        own(15)
    with jax.named_scope("z1fin"):
        finish(11)
        own(16)
        own(17)
        partner(4)
    with jax.named_scope("p0relay"):
        relay(12)
    with jax.named_scope("s1fin"):
        finish(10, 1)
        own(14)
        partner(2, (0,))
    with jax.named_scope("relay1"):
        relay(1)
    with jax.named_scope("y0relay"):
        relay(16)
    with jax.named_scope("relay2"):
        relay(2)
    with jax.named_scope("wave1"):
        wave_in(1).wait_recv()
        own(6)
    with jax.named_scope("y1relay"):
        relay(17)
        for core in range(2):
            wave_far(3, core).start()
        for core in range(2):
            wave_far(4, core).start()
    with jax.named_scope("relay3"):
        relay(3)
    with jax.named_scope("relay5"):
        relay(5)
    with jax.named_scope("p1relay"):
        relay(13)
    with jax.named_scope("p0fin"):
        finish(12)
        partner(0)
    with jax.named_scope("y0fin"):
        finish(16)
        partner(5)
    with jax.named_scope("p3relay"):
        relay(15)
    with jax.named_scope("relay4"):
        relay(4)
    with jax.named_scope("p2relay"):
        relay(14)
    with jax.named_scope("relay6"):
        relay(6)
    with jax.named_scope("wave2"):
        wave_in(2).wait_recv()
        own(7)
    with jax.named_scope("p1fin"):
        finish(13)
        partner(1)
    with jax.named_scope("y1fin"):
        finish(17)
        partner(6)
    with jax.named_scope("p3fin"):
        finish(15)
        partner(3)
    with jax.named_scope("wave3"):
        wave_in(3).wait_recv()
        own(8)
    with jax.named_scope("p2fin"):
        finish(14, 0)
        partner(2, (1,3))
        finish(14, 1)
        partner(2, (2,))
    with jax.named_scope("relay7"):
        relay(7)
    with jax.named_scope("fw0"):
        finish_wave(0)
    with jax.named_scope("wave4"):
        wave_in(4).wait_recv()
        own(9)
    with jax.named_scope("from"):
        bytes_in(rt.at[1 - c], half_sem.at[0])
    with jax.named_scope("b01F"):
        blocks((0,1,), far)
    with jax.named_scope("relay8"):
        relay(8)
    with jax.named_scope("b01N"):
        blocks((0,1,), near)
    with jax.named_scope("relay9"):
        relay(9)
    with jax.named_scope("fw1"):
        finish_wave(1)
    with jax.named_scope("b2F"):
        blocks((2,), far)
    with jax.named_scope("b2N"):
        blocks((2,), near)
    with jax.named_scope("fw2"):
        finish_wave(2)
    with jax.named_scope("b3F"):
        blocks((3,), far)
    with jax.named_scope("fw3"):
        finish_wave(3)
    with jax.named_scope("b4F"):
        blocks((4,), far)
    with jax.named_scope("b34N"):
        blocks((3,4,), near)

    with jax.named_scope("density"):
        for k in range(NK):
            dsend[k : k + 1, :] = jnp.sum(dpart[k], axis=0, keepdims=True)
        dslot[band] = dsend[...]
        for d in range(1, 16):
            density_copy(d).start()

    with jax.named_scope("drain"):
        bytes_out(wave.at[:, pl.ds(0, 640)], out_sem.at[PARTNER_WAVE])
        bytes_out(wave.at[:, pl.ds(0, 1280)], out_sem.at[FAR_WAVE])
        bytes_out(w.at[0, pl.ds(0, 192)], out_sem.at[SCATTER])
        bytes_out(stage.at[pl.ds(0, 3)], out_sem.at[SPREAD])
        bytes_out(w.at[:, pl.ds(0, 1536)], out_sem.at[RING_X])
        bytes_out(w.at[:, pl.ds(0, 1536)], out_sem.at[RING_YZ])
        bytes_out(rt.at[c], out_sem.at[CORE])
        bytes_out(occ_rows.at[pl.ds(0, 3)], out_sem.at[OCC])

    with jax.named_scope("density_in"):
        bytes_in(dslot.at[pl.ds(0, 15)], in_sem.at[DENSITY])
        for g in range(4):
            total = dslot[g] + dslot[4 + g] + dslot[8 + g] + dslot[12 + g]
            dens[g * NK : (g + 1) * NK, :] = total[:NK] * (1.0 / NB)

    with jax.named_scope("out_in"):
        bytes_in(out.at[:, pl.ds(0, 1920)], in_sem.at[RESULT])
        few = out.at[:, pl.ds(0, 640)]
        pltpu.make_async_copy(few, few, in_sem.at[OWN_RESULT]).wait()
    with jax.named_scope("out_sent"):
        bytes_out(out.at[:, pl.ds(0, 1920)], out_sem.at[RESULT])
        bytes_out(dslot.at[pl.ds(0, 15)], out_sem.at[DENSITY])


def store(rotated, density, rotated_out, density_out, sem):
    copies = [pltpu.make_async_copy(density, density_out, sem.at[8])]
    for i in range(8):
        rows = pl.ds(i * 32, 32)
        copies.append(
            pltpu.make_async_copy(rotated.at[rows], rotated_out.at[rows], sem.at[i])
        )
    for copy in copies:
        copy.start()
    for copy in copies:
        copy.wait()


def per_device(wave, ritz, occupation):
    wave, ritz, occ = (
        pltpu.with_memory_space_constraint(a, pltpu.HBM)
        for a in (wave, ritz, occupation.reshape(1, 256))
    )
    dma = pltpu.SemaphoreType.DMA
    vmem = pl.BlockSpec(memory_space=pltpu.VMEM)
    anywhere = pl.BlockSpec(memory_space=pl.ANY)
    rotated, density = pl.pallas_call(
        kernel,
        out_shape=(
            jax.ShapeDtypeStruct((256, 2560), BF16),
            jax.ShapeDtypeStruct((20, 128), F32),
        ),
        in_specs=[pl.BlockSpec(memory_space=pltpu.HBM)] * 3,
        out_specs=(anywhere, vmem),
        scratch_shapes=[
            pltpu.VMEM((256, 512), BF16),
            pltpu.VMEM((1, 256), F32),
            pltpu.VMEM((2, 4, 4, 16, 256), BF16),
            pltpu.VMEM((4, 4, 16, 512), BF16),
            pltpu.VMEM((2, 4, 4, 4, 16, 2048), BF16),
            pltpu.VMEM((2, 2048, 640), BF16),
            pltpu.VMEM((NK, 4, 256, 128), BF16),
            pltpu.VMEM((4, 8, 256), F32),
            pltpu.VMEM((4, 256, 128), F32),
            pltpu.VMEM((NK, 8, 128), F32),
            pltpu.VMEM((8, 128), F32),
            pltpu.VMEM((16, 8, 128), F32),
            dma((11,)), dma((11,)), dma((NK,)), dma((46,)), dma((6,)),
        ],
        compiler_params=pltpu.CompilerParams(
            has_side_effects=True, collective_id=0, vmem_limit_bytes=VM
        ),
        name="rotate",
    )(wave, ritz, occ)
    rotated, density = pl.pallas_call(
        store,
        out_shape=(
            jax.ShapeDtypeStruct((256, 2560), BF16),
            jax.ShapeDtypeStruct((20, 128), F32),
        ),
        in_specs=[anywhere, anywhere],
        out_specs=[pl.BlockSpec(memory_space=pltpu.HBM)] * 2,
        scratch_shapes=[dma((9,))],
        compiler_params=pltpu.CompilerParams(vmem_limit_bytes=1024 * 1024),
        name="store",
    )(rotated, density)
    return rotated, density.reshape(2560)


def solution(mesh):
    return jax.shard_map(
        per_device,
        mesh=mesh,
        in_specs=(P("band", "grid"), P("band", "grid"), P("band")),
        out_specs=(P("band", "grid"), P("grid")),
        check_vma=False,
    )
```

```python
import jax
import jax.numpy as jnp
from jax import lax
from jax.experimental import pallas as pl
from jax.experimental.pallas import tpu as pltpu
from jax.sharding import PartitionSpec as P

NB = 4096
MESH = pl.DeviceIdType.MESH
F32, BF16 = jnp.float32, jnp.bfloat16

VM = 24 * 1024 * 1024
NK = 5
CA = 1408

N_RINGS = 18

PARTNER_WAVE, FAR_WAVE, SCATTER, SPREAD, RING_X, RING_YZ, CORE, OCC, RESULT, DENSITY, LOCAL = range(11)
OWN_RESULT, RITZ, OCC_HERE = RING_X, RING_YZ, CORE

def hops(*steps):
    return sum(min(step, 4 - step) for step in steps)


IN_PLANE = sorted(
    ((hops(dy, dz), dy, dz) for dy in range(4) for dz in range(4) if dy or dz),
    key=lambda d: -d[0],
)
SHARERS = [
    (hops(dx, dy), dx, dy, dc)
    for dx in range(4) for dy in (0, 2) for dc in range(2)
    if (dx, dy, dc) not in ((0, 0, 0), (0, 2, 0))
]


def at(x, y, z, core):
    return (x * 4 + (y // 2) * 2 + core, (y % 2) * 4 + z)


def kernel(
    wave, ritz, occ, out, dens,
    ritz_here, occ_here, rt_src, stage, rt, w, cbuf, occ_rows, occ_cols, dpart, dsend, dslot,
    out_sem, in_sem, wave_sem, ring_sem, half_sem,
):
    band, grid = lax.axis_index("band"), lax.axis_index("grid")
    x, yhi, c = band // 4, (band // 2) % 2, band % 2
    ylo, z = grid // 4, grid % 4
    y = yhi * 2 + ylo
    xj = 2 * ylo + z // 2
    zb = z % 2
    mine = yhi * 2 + c
    near, far = yhi, 1 - yhi

    def many(n, i):
        return pl.ds(pl.multiple_of(i * n, n), n)

    def send(src, dst, send_sem, recv_sem, device):
        return pltpu.make_async_remote_copy(
            src_ref=src, dst_ref=dst, send_sem=send_sem, recv_sem=recv_sem,
            device_id=device, device_id_type=MESH,
        )

    def cells(k):
        return pl.ds(k * 128, 128)

    def wave_local():
        return pltpu.make_async_copy(
            wave.at[:, many(640, yhi * 2 + c)], w.at[c, many(256, x * 2 + near)], in_sem.at[LOCAL]
        )

    def wave_partner(p):
        first, n = ((0, 128), (128, 512))[p]
        col = pl.multiple_of((yhi * 2 + 1 - c) * 640 + first, 128)
        return send(
            wave.at[:, pl.ds(col, n)], w.at[c, many(256, x * 2 + near), pl.ds(first, n)],
            out_sem.at[PARTNER_WAVE], half_sem.at[1] if p else in_sem.at[PARTNER_WAVE],
            at(x, y, z, 1 - c),
        )

    def wave_far(k, core):
        col = pl.multiple_of((1 - yhi) * 1280 + core * 640 + k * 128, 128)
        return send(
            wave.at[:, pl.ds(col, 128)],
            w.at[c, many(256, x * 2 + near), cells(k)],
            out_sem.at[FAR_WAVE], wave_sem.at[k], at(x, (y + 2) % 4, z, core),
        )

    def wave_in(k):
        rows = w.at[:, many(256, x * 2 + far), cells(k)]
        return send(rows, rows, out_sem.at[FAR_WAVE], wave_sem.at[k], at(x, (y + 2) % 4, z, c))

    def scatter(dy, dz):
        yp, zp = (y + dy) % 4, (z + dz) % 4
        return send(
            rt_src.at[:, zp, yp],
            stage.at[xj, many(2, zb), :, many(256, yhi)],
            out_sem.at[SCATTER], in_sem.at[SCATTER], at(x, yp, zp, c),
        )

    def spread(d):
        other = (x + d) % 4
        return send(
            stage.at[other], rt.at[c, :, z, y, :, many(512, x)],
            out_sem.at[SPREAD], in_sem.at[SPREAD], at(other, y, z, c),
        )

    def ring(i):
        if i < 10:
            k, rows = i % 5, (near if i < 5 else far)
            block = lambda v, h: w.at[h, many(256, v * 2 + rows), cells(k)]
        elif i == 10:
            block = lambda v, h: rt.at[c, pl.ds(h * 2, 2), z, v, :, pl.ds(0, CA)]
        elif i == 11:
            block = lambda v, h: rt.at[c, pl.ds(h * 2, 2), v, y, :, pl.ds(CA, 2048 - CA)]
        elif i < 16:
            block = lambda v, h: rt.at[c, pl.ds(h * 2, 2), v, (y + i - 12) % 4, :, pl.ds(0, CA)]
        else:
            n = 2048 - CA
            block = lambda v, h: rt.at[c, pl.ds((i - 16) * 2, 2), pl.ds(h * 2, 2), v, :, pl.ds(CA, n)]
        return block

    def sem_of(i, n):
        if n == 2:
            return 26 + (i == 14)
        return i if i < 10 else 10 + (i - 10) * 2 + n

    def ring_copy(i, j, v, h):
        block, slot = ring(i), i
        axis = "x" if i < 10 else "y" if i in (10, 16, 17) else "z"
        to = 1 if j < 3 else 3
        if axis == "x":
            me, device = x, at((x + to) % 4, y, z, c)
        elif axis == "y":
            me, device = y, at(x, (y + to) % 4, z, c)
        else:
            me, device = z, at(x, y, (z + to) % 4, c)
        ref = block((me + v) % 4, h)
        sent = out_sem.at[RING_X if axis == "x" else RING_YZ]
        if j in (0, 3):
            got = ring_sem.at[sem_of(slot, 0)]
        elif axis == "x":
            got = half_sem.at[2 + max(slot % 5 - 1, 0)]
        else:
            got = ring_sem.at[sem_of(slot, 2 if slot in (10, 14) and j in (2, 5) else 1)]
        return send(ref, ref, sent, got, device)

    def own_first(i):
        ring_copy(i, 0, 0, 0).start()
        ring_copy(i, 3, 0, 1).start()

    def own_rest(i):
        ring_copy(i, 1, 0, 1).start()
        ring_copy(i, 4, 0, 0).start()

    def own(i):
        own_first(i)
        own_rest(i)

    def relay(i):
        if i < 10:
            ref = rt.at[0, 0, 0, pl.ds(0, 2)]
        elif i in (16, 17):
            ref = rt.at[c, pl.ds(0, 2), :, 0, :, pl.ds(CA, 2048 - CA)]
        else:
            ref = rt.at[c, :, 0, 0, :, pl.ds(CA, 2048 - CA) if i == 11 else pl.ds(0, CA)]
        bytes_in(ref, ring_sem.at[sem_of(i, 0)])
        ring_copy(i, 2, 3, 0).start()
        ring_copy(i, 5, 1, 1).start()

    def bytes_in(ref, sem):
        send(ref, ref, out_sem.at[0], sem, at(x, y, z, 1 - c)).wait_recv()

    def bytes_out(ref, sem):
        send(ref, ref, sem, in_sem.at[0], at(x, y, z, 1 - c)).wait_send()

    def finish(i, part=0):
        low, high = pl.ds(0, CA), pl.ds(CA, 2048 - CA)
        if i in (10, 14):
            bytes_in(rt.at[c, :, 0, 0, :, low], ring_sem.at[sem_of(i, 1 + part)])
        elif i == 11:
            bytes_in(rt.at[c, :, pl.ds(0, 2), 0, :, high], ring_sem.at[sem_of(i, 1)])
        elif i < 16:
            bytes_in(rt.at[c, :, pl.ds(0, 2), 0, :, low], ring_sem.at[sem_of(i, 1)])
        else:
            bytes_in(rt.at[c, pl.ds(0, 2), :, pl.ds(0, 2), :, high], ring_sem.at[sem_of(i, 1)])

    def finish_wave(g):
        bytes_in(rt.at[0, 0, pl.ds(0, 2 if g else 4)], half_sem.at[2 + g])

    def to_core(ref, sem):
        send(ref, ref, out_sem.at[CORE], half_sem.at[sem], at(x, y, z, 1 - c)).start()

    def partner(half, d, vs=None):
        for v in vs or (None,):
            planes = slice(None) if v is None else (z + v) % 4
            to_core(
                rt.at[c, many(2, half), planes, (y + d) % 4, :, pl.ds(0, CA)], 6 if half is near else 0
            )

    def partner_rest(half, ds):
        for d in ds:
            ref = rt.at[c, pl.ds(half * 2, 2), :, (y + d) % 4, :, pl.ds(CA, 2048 - CA)]
            to_core(ref, ((half + far) % 2) * 6)

    def occ_copy(d, src=False):
        yy = y if d == 0 else (y + 2) % 4
        cc = c if d == 1 else 1 - c
        row = (yy // 2) * 2 + cc if src else mine
        return send(
            occ_rows.at[mine], occ_rows.at[row], out_sem.at[OCC], in_sem.at[OCC], at(x, yy, z, cc)
        )

    def result(k, hi, core):
        return send(
            cbuf.at[k, hi * 2 + core], out.at[:, many(128, yhi * 10 + c * 5 + k)],
            out_sem.at[RESULT], in_sem.at[RESULT], at(x, hi * 2 + ylo, z, core),
        )

    def result_here(k):
        return pltpu.make_async_copy(
            cbuf.at[k, mine], out.at[:, many(128, yhi * 10 + c * 5 + k)], in_sem.at[OWN_RESULT]
        )

    def density_copy(d):
        to = at((x + d // 4) % 4, (y + 2 * ((d // 2) % 2)) % 4, z, (c + d) % 2)
        return send(dsend, dslot.at[band], out_sem.at[DENSITY], in_sem.at[DENSITY], to)

    def take(k, s, summed):
        rounded = summed.astype(BF16)
        cbuf[k, s] = rounded
        values = rounded.astype(F32)
        terms = occ_cols[s] * values * values
        dpart[k] += terms.reshape(32, 8, 128).sum(axis=0)

    def product(s, ks):
        cols = pl.ds(ks[0] * 128, 128 * len(ks))
        parts = [
            jnp.dot(
                rt[v, s].reshape(256, 2048), w[v, :, cols], preferred_element_type=F32
            )
            for v in range(2)
        ]
        return parts[0] + parts[1]

    def blocks(ks, hi):
        @pl.loop(0, 2)
        def _(core):
            s = hi * 2 + core
            summed = product(s, ks)
            for n, k in enumerate(ks):
                take(k, s, summed[:, n * 128 : (n + 1) * 128])
            if hi is far:
                for k in ks:
                    result(k, hi, core).start()

        if hi is near:
            for k in ks:
                result(k, hi, 1 - c).start()
            for k in ks:
                result_here(k).start()

    with jax.named_scope("signal"):
        peers = [(n, at((x + dx) % 4, (y + dy) % 4, z, (c + dc) % 2)) for n, dx, dy, dc in SHARERS]
        peers += [(n, at(x, (y + dy) % 4, (z + dz) % 4, c)) for n, dy, dz in IN_PLANE]
        peers = [peer for _, peer in sorted(peers, key=lambda p: -p[0])]
        barrier = pltpu.get_barrier_semaphore()
        for peer in peers:
            pl.semaphore_signal(barrier, inc=1, device_id=peer, device_id_type=MESH)
        load_ritz = pltpu.make_async_copy(ritz, ritz_here, in_sem.at[RITZ])
        load_occ = pltpu.make_async_copy(occ, occ_here, in_sem.at[OCC_HERE])
        load_ritz.start()
        load_occ.start()
        wave_local().start()

    with jax.named_scope("transpose"):
        load_ritz.wait()
        load_occ.wait()
        rt_src[...] = ritz_here[...].T.reshape(2, 4, 4, 16, 256)
        occ_rows[mine] = jnp.broadcast_to(occ_here[...], (8, 256))
        stage[xj, many(2, zb), :, many(256, yhi)] = rt_src[:, z, y]
        dpart[...] = jnp.zeros_like(dpart)
        dsend[...] = jnp.zeros_like(dsend)
    with jax.named_scope("barrier"):
        pl.semaphore_wait(barrier, len(peers))

    with jax.named_scope("start"):
        for _, dy, dz in IN_PLANE:
            scatter(dy, dz).start()
        wave_local().wait()
        for p in range(2):
            wave_partner(p).start()
        for d in range(3):
            occ_copy(d).start()
    with jax.named_scope("pw"):
        bytes_in(wave.at[:, pl.ds(0, 128)], in_sem.at[PARTNER_WAVE])
        own(0)
        bytes_in(wave.at[:, pl.ds(0, 512)], half_sem.at[1])
    with jax.named_scope("scin"):
        bytes_in(w.at[0, pl.ds(0, 192)], in_sem.at[SCATTER])
        for d in (2, 1, 3):
            spread(d).start()
        rt[c, :, z, y, :, many(512, x)] = stage[x]
        for core in range(2):
            wave_far(0, core).start()
        for core in range(2):
            wave_far(1, core).start()
        own(1)
        own(2)
        own(3)
        own(4)
    with jax.named_scope("spin"):
        bytes_in(stage.at[pl.ds(0, 3)], in_sem.at[SPREAD])
        own(11)
        own(12)
        own(10)
    with jax.named_scope("occ"):
        bytes_in(occ_rows.at[pl.ds(0, 3)], in_sem.at[OCC])
        for s in range(4):
            occ_cols[s] = jnp.broadcast_to(occ_rows[s][0:1, :], (128, 256)).T
    with jax.named_scope("s1relay"):
        relay(10)
        relay(11)
        for core in range(2):
            wave_far(2, core).start()
    with jax.named_scope("relay0"):
        relay(0)
    with jax.named_scope("wave0"):
        wave_in(0).wait_recv()
        own(5)
    with jax.named_scope("finA"):
        finish(10, 0)
        own(13)
        own(15)
    with jax.named_scope("z1fin"):
        finish(11)
        own(16)
        own(17)
        partner_rest(0, (0,))
        partner_rest(1, (0,))
    with jax.named_scope("p0relay"):
        relay(12)
    with jax.named_scope("s1fin"):
        finish(10, 1)
        own(14)
        partner(far, 2, (0,))
        partner(near, 2, (0,))
    with jax.named_scope("relay1"):
        relay(1)
    with jax.named_scope("y0relay"):
        relay(16)
    with jax.named_scope("relay2"):
        relay(2)
    with jax.named_scope("wave1"):
        wave_in(1).wait_recv()
        own(6)
    with jax.named_scope("y1relay"):
        relay(17)
        for core in range(2):
            wave_far(3, core).start()
        for core in range(2):
            wave_far(4, core).start()
    with jax.named_scope("relay3"):
        relay(3)
    with jax.named_scope("relay5"):
        relay(5)
    with jax.named_scope("p1relay"):
        relay(13)
    with jax.named_scope("p0fin"):
        finish(12)
        partner(far, 0)
        partner(near, 0)
    with jax.named_scope("y0fin"):
        finish(16)
        partner_rest(0, (1,2,3))
    with jax.named_scope("p3relay"):
        relay(15)
    with jax.named_scope("relay4"):
        relay(4)
    with jax.named_scope("p2relay"):
        relay(14)
    with jax.named_scope("relay6"):
        relay(6)
    with jax.named_scope("wave2"):
        wave_in(2).wait_recv()
        own(7)
    with jax.named_scope("p1fin"):
        finish(13)
        partner(far, 1)
        partner(near, 1)
    with jax.named_scope("y1fin"):
        finish(17)
        partner_rest(1, (1,2,3))
    with jax.named_scope("p3fin"):
        finish(15)
        partner(far, 3)
    with jax.named_scope("wave3"):
        wave_in(3).wait_recv()
        own(8)
    with jax.named_scope("p2fin"):
        finish(14, 0)
        partner(far, 2, (1,3))
        finish(14, 1)
        partner(far, 2, (2,))
        partner(near, 3)
        partner(near, 2, (1,2,3))
    with jax.named_scope("relay7"):
        relay(7)
    with jax.named_scope("fw0"):
        finish_wave(0)
    with jax.named_scope("wave4"):
        wave_in(4).wait_recv()
        own(9)
    with jax.named_scope("from"):
        bytes_in(rt.at[1 - c, pl.ds(0, 2)], half_sem.at[0])
    with jax.named_scope("b01F"):
        blocks((0,1,), far)
    with jax.named_scope("relay8"):
        relay(8)
    with jax.named_scope("fromN"):
        bytes_in(rt.at[1 - c, pl.ds(0, 2)], half_sem.at[6])
    with jax.named_scope("b01N"):
        blocks((0,1,), near)
    with jax.named_scope("fw1"):
        finish_wave(1)
    with jax.named_scope("b2F"):
        blocks((2,), far)
    with jax.named_scope("relay9"):
        relay(9)
    with jax.named_scope("b2N"):
        blocks((2,), near)
    with jax.named_scope("fw2"):
        finish_wave(2)
    with jax.named_scope("b3F"):
        blocks((3,), far)
    with jax.named_scope("fw3"):
        finish_wave(3)
    with jax.named_scope("b4F"):
        blocks((4,), far)
    with jax.named_scope("b34N"):
        blocks((3,4,), near)

    with jax.named_scope("density"):
        for k in range(NK):
            dsend[k : k + 1, :] = jnp.sum(dpart[k], axis=0, keepdims=True)
        dslot[band] = dsend[...]
        for d in range(1, 16):
            density_copy(d).start()

    with jax.named_scope("drain"):
        bytes_out(wave.at[:, pl.ds(0, 640)], out_sem.at[PARTNER_WAVE])
        bytes_out(wave.at[:, pl.ds(0, 1280)], out_sem.at[FAR_WAVE])
        bytes_out(w.at[0, pl.ds(0, 192)], out_sem.at[SCATTER])
        bytes_out(stage.at[pl.ds(0, 3)], out_sem.at[SPREAD])
        bytes_out(w.at[:, pl.ds(0, 1536)], out_sem.at[RING_X])
        bytes_out(w.at[:, pl.ds(0, 1536)], out_sem.at[RING_YZ])
        bytes_out(rt.at[c], out_sem.at[CORE])
        bytes_out(occ_rows.at[pl.ds(0, 3)], out_sem.at[OCC])

    with jax.named_scope("density_in"):
        bytes_in(dslot.at[pl.ds(0, 15)], in_sem.at[DENSITY])
        for g in range(4):
            total = dslot[g] + dslot[4 + g] + dslot[8 + g] + dslot[12 + g]
            dens[g * NK : (g + 1) * NK, :] = total[:NK] * (1.0 / NB)

    with jax.named_scope("out_in"):
        bytes_in(out.at[:, pl.ds(0, 1920)], in_sem.at[RESULT])
        few = out.at[:, pl.ds(0, 640)]
        pltpu.make_async_copy(few, few, in_sem.at[OWN_RESULT]).wait()
    with jax.named_scope("out_sent"):
        bytes_out(out.at[:, pl.ds(0, 1920)], out_sem.at[RESULT])
        bytes_out(dslot.at[pl.ds(0, 15)], out_sem.at[DENSITY])


def store(rotated, density, rotated_out, density_out, sem):
    copies = [pltpu.make_async_copy(density, density_out, sem.at[8])]
    for i in range(8):
        rows = pl.ds(i * 32, 32)
        copies.append(
            pltpu.make_async_copy(rotated.at[rows], rotated_out.at[rows], sem.at[i])
        )
    for copy in copies:
        copy.start()
    for copy in copies:
        copy.wait()


def per_device(wave, ritz, occupation):
    wave, ritz, occ = (
        pltpu.with_memory_space_constraint(a, pltpu.HBM)
        for a in (wave, ritz, occupation.reshape(1, 256))
    )
    dma = pltpu.SemaphoreType.DMA
    vmem = pl.BlockSpec(memory_space=pltpu.VMEM)
    anywhere = pl.BlockSpec(memory_space=pl.ANY)
    rotated, density = pl.pallas_call(
        kernel,
        out_shape=(
            jax.ShapeDtypeStruct((256, 2560), BF16),
            jax.ShapeDtypeStruct((20, 128), F32),
        ),
        in_specs=[pl.BlockSpec(memory_space=pltpu.HBM)] * 3,
        out_specs=(anywhere, vmem),
        scratch_shapes=[
            pltpu.VMEM((256, 512), BF16),
            pltpu.VMEM((1, 256), F32),
            pltpu.VMEM((2, 4, 4, 16, 256), BF16),
            pltpu.VMEM((4, 4, 16, 512), BF16),
            pltpu.VMEM((2, 4, 4, 4, 16, 2048), BF16),
            pltpu.VMEM((2, 2048, 640), BF16),
            pltpu.VMEM((NK, 4, 256, 128), BF16),
            pltpu.VMEM((4, 8, 256), F32),
            pltpu.VMEM((4, 256, 128), F32),
            pltpu.VMEM((NK, 8, 128), F32),
            pltpu.VMEM((8, 128), F32),
            pltpu.VMEM((16, 8, 128), F32),
            dma((11,)), dma((11,)), dma((NK,)), dma((28,)), dma((7,)),
        ],
        compiler_params=pltpu.CompilerParams(
            has_side_effects=True, collective_id=0, vmem_limit_bytes=VM
        ),
        name="rotate",
    )(wave, ritz, occ)
    rotated, density = pl.pallas_call(
        store,
        out_shape=(
            jax.ShapeDtypeStruct((256, 2560), BF16),
            jax.ShapeDtypeStruct((20, 128), F32),
        ),
        in_specs=[anywhere, anywhere],
        out_specs=[pl.BlockSpec(memory_space=pltpu.HBM)] * 2,
        scratch_shapes=[dma((9,))],
        compiler_params=pltpu.CompilerParams(vmem_limit_bytes=1024 * 1024),
        name="store",
    )(rotated, density)
    return rotated, density.reshape(2560)


def solution(mesh):
    return jax.shard_map(
        per_device,
        mesh=mesh,
        in_specs=(P("band", "grid"), P("band", "grid"), P("band")),
        out_specs=(P("band", "grid"), P("grid")),
        check_vma=False,
    )
```

```python
import jax
import jax.numpy as jnp
from jax import lax
from jax.experimental import pallas as pl
from jax.experimental.pallas import tpu as pltpu
from jax.sharding import PartitionSpec as P

NB = 4096
MESH = pl.DeviceIdType.MESH
F32, BF16 = jnp.float32, jnp.bfloat16

VM = 24 * 1024 * 1024
NK = 5
CA = 1408

N_RINGS = 18

PARTNER_WAVE, FAR_WAVE, SCATTER, SPREAD, RING_X, RING_YZ, CORE, OCC, RESULT, DENSITY, LOCAL = range(11)
OWN_RESULT, RITZ, OCC_HERE = RING_X, RING_YZ, CORE

def hops(*steps):
    return sum(min(step, 4 - step) for step in steps)


IN_PLANE = sorted(
    ((hops(dy, dz), dy, dz) for dy in range(4) for dz in range(4) if dy or dz),
    key=lambda d: -d[0],
)
SHARERS = [
    (hops(dx, dy), dx, dy, dc)
    for dx in range(4) for dy in (0, 2) for dc in range(2)
    if (dx, dy, dc) not in ((0, 0, 0), (0, 2, 0))
]


def at(x, y, z, core):
    return (x * 4 + (y // 2) * 2 + core, (y % 2) * 4 + z)


def kernel(
    wave, ritz, occ, out, dens,
    ritz_here, occ_here, rt_src, stage, rt, w, cbuf, occ_rows, occ_cols, dpart, dsend, dslot,
    out_sem, in_sem, wave_sem, ring_sem, half_sem,
):
    band, grid = lax.axis_index("band"), lax.axis_index("grid")
    x, yhi, c = band // 4, (band // 2) % 2, band % 2
    ylo, z = grid // 4, grid % 4
    y = yhi * 2 + ylo
    xj = 2 * ylo + z // 2
    zb = z % 2
    mine = yhi * 2 + c
    near, far = yhi, 1 - yhi

    def many(n, i):
        return pl.ds(pl.multiple_of(i * n, n), n)

    def send(src, dst, send_sem, recv_sem, device):
        return pltpu.make_async_remote_copy(
            src_ref=src, dst_ref=dst, send_sem=send_sem, recv_sem=recv_sem,
            device_id=device, device_id_type=MESH,
        )

    def cells(k):
        return pl.ds(k * 128, 128)

    def wave_local():
        return pltpu.make_async_copy(
            wave.at[:, many(640, yhi * 2 + c)], w.at[c, many(256, x * 2 + near)], in_sem.at[LOCAL]
        )

    def wave_partner(p):
        first, n = ((0, 128), (128, 512))[p]
        col = pl.multiple_of((yhi * 2 + 1 - c) * 640 + first, 128)
        return send(
            wave.at[:, pl.ds(col, n)], w.at[c, many(256, x * 2 + near), pl.ds(first, n)],
            out_sem.at[PARTNER_WAVE], half_sem.at[1] if p else in_sem.at[PARTNER_WAVE],
            at(x, y, z, 1 - c),
        )

    def wave_far(k, core):
        col = pl.multiple_of((1 - yhi) * 1280 + core * 640 + k * 128, 128)
        return send(
            wave.at[:, pl.ds(col, 128)],
            w.at[c, many(256, x * 2 + near), cells(k)],
            out_sem.at[FAR_WAVE], wave_sem.at[k], at(x, (y + 2) % 4, z, core),
        )

    def wave_in(k):
        rows = w.at[:, many(256, x * 2 + far), cells(k)]
        return send(rows, rows, out_sem.at[FAR_WAVE], wave_sem.at[k], at(x, (y + 2) % 4, z, c))

    def scatter(dy, dz):
        yp, zp = (y + dy) % 4, (z + dz) % 4
        return send(
            rt_src.at[:, zp, yp],
            stage.at[xj, many(2, zb), :, many(256, yhi)],
            out_sem.at[SCATTER], in_sem.at[SCATTER], at(x, yp, zp, c),
        )

    def spread(d):
        other = (x + d) % 4
        return send(
            stage.at[other], rt.at[c, :, z, y, :, many(512, x)],
            out_sem.at[SPREAD], in_sem.at[SPREAD], at(other, y, z, c),
        )

    def ring(i):
        if i < 10:
            k, rows = i % 5, (near if i < 5 else far)
            block = lambda v, h: w.at[h, many(256, v * 2 + rows), cells(k)]
        elif i == 10:
            block = lambda v, h: rt.at[c, pl.ds(h * 2, 2), z, v, :, pl.ds(0, CA)]
        elif i == 11:
            block = lambda v, h: rt.at[c, pl.ds(h * 2, 2), v, y, :, pl.ds(CA, 2048 - CA)]
        elif i < 16:
            block = lambda v, h: rt.at[c, pl.ds(h * 2, 2), v, (y + i - 12) % 4, :, pl.ds(0, CA)]
        else:
            n = 2048 - CA
            block = lambda v, h: rt.at[c, pl.ds((i - 16) * 2, 2), pl.ds(h * 2, 2), v, :, pl.ds(CA, n)]
        return block

    def sem_of(i, n):
        if n == 2:
            return 26 + (i == 14)
        return i if i < 10 else 10 + (i - 10) * 2 + n

    def ring_copy(i, j, v, h):
        block, slot = ring(i), i
        axis = "x" if i < 10 else "y" if i in (10, 16, 17) else "z"
        to = 1 if j < 3 else 3
        if axis == "x":
            me, device = x, at((x + to) % 4, y, z, c)
        elif axis == "y":
            me, device = y, at(x, (y + to) % 4, z, c)
        else:
            me, device = z, at(x, y, (z + to) % 4, c)
        ref = block((me + v) % 4, h)
        sent = out_sem.at[RING_X if axis == "x" else RING_YZ]
        if j in (0, 3):
            got = ring_sem.at[sem_of(slot, 0)]
        elif axis == "x":
            got = half_sem.at[2 + max(slot % 5 - 1, 0)]
        else:
            got = ring_sem.at[sem_of(slot, 2 if slot in (10, 14) and j in (2, 5) else 1)]
        return send(ref, ref, sent, got, device)

    def own_first(i):
        ring_copy(i, 0, 0, 0).start()
        ring_copy(i, 3, 0, 1).start()

    def own_rest(i):
        ring_copy(i, 1, 0, 1).start()
        ring_copy(i, 4, 0, 0).start()

    def own(i):
        own_first(i)
        own_rest(i)

    def relay(i):
        if i < 10:
            ref = rt.at[0, 0, 0, pl.ds(0, 2)]
        elif i in (16, 17):
            ref = rt.at[c, pl.ds(0, 2), :, 0, :, pl.ds(CA, 2048 - CA)]
        else:
            ref = rt.at[c, :, 0, 0, :, pl.ds(CA, 2048 - CA) if i == 11 else pl.ds(0, CA)]
        bytes_in(ref, ring_sem.at[sem_of(i, 0)])
        ring_copy(i, 2, 3, 0).start()
        ring_copy(i, 5, 1, 1).start()

    def bytes_in(ref, sem):
        send(ref, ref, out_sem.at[0], sem, at(x, y, z, 1 - c)).wait_recv()

    def bytes_out(ref, sem):
        send(ref, ref, sem, in_sem.at[0], at(x, y, z, 1 - c)).wait_send()

    def finish(i, part=0):
        low, high = pl.ds(0, CA), pl.ds(CA, 2048 - CA)
        if i in (10, 14):
            bytes_in(rt.at[c, :, 0, 0, :, low], ring_sem.at[sem_of(i, 1 + part)])
        elif i == 11:
            bytes_in(rt.at[c, :, pl.ds(0, 2), 0, :, high], ring_sem.at[sem_of(i, 1)])
        elif i < 16:
            bytes_in(rt.at[c, :, pl.ds(0, 2), 0, :, low], ring_sem.at[sem_of(i, 1)])
        else:
            bytes_in(rt.at[c, pl.ds(0, 2), :, pl.ds(0, 2), :, high], ring_sem.at[sem_of(i, 1)])

    def finish_wave(g):
        bytes_in(rt.at[0, 0, pl.ds(0, 2 if g else 4)], half_sem.at[2 + g])

    def partner(p, vs=()):
        if p == 2:
            refs = [rt.at[c, :, (z + v) % 4, (y + 2) % 4, :, pl.ds(0, CA)] for v in vs]
        elif p < 4:
            refs = [rt.at[c, :, :, (y + p) % 4, :, pl.ds(0, CA)]]
        elif p == 4:
            refs = [rt.at[c, :, :, y, :, pl.ds(CA, 2048 - CA)]]
        else:
            refs = [
                rt.at[c, pl.ds((p - 5) * 2, 2), :, (y + d) % 4, :, pl.ds(CA, 2048 - CA)]
                for d in range(1, 4)
            ]
        for ref in refs:
            send(ref, ref, out_sem.at[CORE], half_sem.at[0], at(x, y, z, 1 - c)).start()

    def occ_copy(d, src=False):
        yy = y if d == 0 else (y + 2) % 4
        cc = c if d == 1 else 1 - c
        row = (yy // 2) * 2 + cc if src else mine
        return send(
            occ_rows.at[mine], occ_rows.at[row], out_sem.at[OCC], in_sem.at[OCC], at(x, yy, z, cc)
        )

    def result(k, hi, core):
        return send(
            cbuf.at[k, hi * 2 + core], out.at[:, many(128, yhi * 10 + c * 5 + k)],
            out_sem.at[RESULT], in_sem.at[RESULT], at(x, hi * 2 + ylo, z, core),
        )

    def result_here(k):
        return pltpu.make_async_copy(
            cbuf.at[k, mine], out.at[:, many(128, yhi * 10 + c * 5 + k)], in_sem.at[OWN_RESULT]
        )

    def density_copy(d):
        to = at((x + d // 4) % 4, (y + 2 * ((d // 2) % 2)) % 4, z, (c + d) % 2)
        return send(dsend, dslot.at[band], out_sem.at[DENSITY], in_sem.at[DENSITY], to)

    def take(k, s, summed):
        rounded = summed.astype(BF16)
        cbuf[k, s] = rounded
        values = rounded.astype(F32)
        terms = occ_cols[s] * values * values
        dpart[k] += terms.reshape(32, 8, 128).sum(axis=0)

    def product(s, ks):
        cols = pl.ds(ks[0] * 128, 128 * len(ks))
        parts = [
            jnp.dot(
                rt[v, s].reshape(256, 2048), w[v, :, cols], preferred_element_type=F32
            )
            for v in range(2)
        ]
        return parts[0] + parts[1]

    def blocks(ks, hi):
        @pl.loop(0, 2)
        def _(core):
            s = hi * 2 + core
            summed = product(s, ks)
            for n, k in enumerate(ks):
                take(k, s, summed[:, n * 128 : (n + 1) * 128])
            if hi is far:
                for k in ks:
                    result(k, hi, core).start()

        if hi is near:
            for k in ks:
                result(k, hi, 1 - c).start()
            for k in ks:
                result_here(k).start()

    with jax.named_scope("signal"):
        peers = [(n, at((x + dx) % 4, (y + dy) % 4, z, (c + dc) % 2)) for n, dx, dy, dc in SHARERS]
        peers += [(n, at(x, (y + dy) % 4, (z + dz) % 4, c)) for n, dy, dz in IN_PLANE]
        peers = [peer for _, peer in sorted(peers, key=lambda p: -p[0])]
        barrier = pltpu.get_barrier_semaphore()
        for peer in peers:
            pl.semaphore_signal(barrier, inc=1, device_id=peer, device_id_type=MESH)
        load_ritz = pltpu.make_async_copy(ritz, ritz_here, in_sem.at[RITZ])
        load_occ = pltpu.make_async_copy(occ, occ_here, in_sem.at[OCC_HERE])
        load_ritz.start()
        load_occ.start()
        wave_local().start()

    with jax.named_scope("transpose"):
        load_ritz.wait()
        load_occ.wait()
        rt_src[...] = ritz_here[...].T.reshape(2, 4, 4, 16, 256)
        occ_rows[mine] = jnp.broadcast_to(occ_here[...], (8, 256))
        stage[xj, many(2, zb), :, many(256, yhi)] = rt_src[:, z, y]
        dpart[...] = jnp.zeros_like(dpart)
        dsend[...] = jnp.zeros_like(dsend)
    with jax.named_scope("barrier"):
        pl.semaphore_wait(barrier, len(peers))

    with jax.named_scope("start"):
        for _, dy, dz in IN_PLANE:
            scatter(dy, dz).start()
        wave_local().wait()
        for p in range(2):
            wave_partner(p).start()
        for d in range(3):
            occ_copy(d).start()
    with jax.named_scope("pw"):
        bytes_in(wave.at[:, pl.ds(0, 128)], in_sem.at[PARTNER_WAVE])
        own(0)
        bytes_in(wave.at[:, pl.ds(0, 512)], half_sem.at[1])
    with jax.named_scope("scin"):
        bytes_in(w.at[0, pl.ds(0, 192)], in_sem.at[SCATTER])
        for d in (2, 1, 3):
            spread(d).start()
        rt[c, :, z, y, :, many(512, x)] = stage[x]
        for core in range(2):
            wave_far(0, core).start()
        for core in range(2):
            wave_far(1, core).start()
        own(1)
        own(2)
        own(3)
        own(4)
    with jax.named_scope("spin"):
        bytes_in(stage.at[pl.ds(0, 3)], in_sem.at[SPREAD])
        own(11)
        own(12)
        own(10)
    with jax.named_scope("occ"):
        bytes_in(occ_rows.at[pl.ds(0, 3)], in_sem.at[OCC])
        for s in range(4):
            occ_cols[s] = jnp.broadcast_to(occ_rows[s][0:1, :], (128, 256)).T
    with jax.named_scope("s1relay"):
        relay(10)
        relay(11)
        for core in range(2):
            wave_far(2, core).start()
    with jax.named_scope("relay0"):
        relay(0)
    with jax.named_scope("wave0"):
        wave_in(0).wait_recv()
        own(5)
    with jax.named_scope("finA"):
        finish(10, 0)
        own(13)
        own(15)
    with jax.named_scope("z1fin"):
        finish(11)
        own(16)
        own(17)
        partner(4)
    with jax.named_scope("p0relay"):
        relay(12)
    with jax.named_scope("s1fin"):
        finish(10, 1)
        own(14)
        partner(2, (0,))
    with jax.named_scope("relay1"):
        relay(1)
    with jax.named_scope("y0relay"):
        relay(16)
    with jax.named_scope("relay2"):
        relay(2)
    with jax.named_scope("wave1"):
        wave_in(1).wait_recv()
        own(6)
    with jax.named_scope("y1relay"):
        relay(17)
        for core in range(2):
            wave_far(3, core).start()
        for core in range(2):
            wave_far(4, core).start()
    with jax.named_scope("relay3"):
        relay(3)
    with jax.named_scope("relay5"):
        relay(5)
    with jax.named_scope("p1relay"):
        relay(13)
    with jax.named_scope("p0fin"):
        finish(12)
        partner(0)
    with jax.named_scope("y0fin"):
        finish(16)
        partner(5)
    with jax.named_scope("p3relay"):
        relay(15)
    with jax.named_scope("relay4"):
        relay(4)
    with jax.named_scope("p2relay"):
        relay(14)
    with jax.named_scope("relay6"):
        relay(6)
    with jax.named_scope("wave2"):
        wave_in(2).wait_recv()
        own(7)
    with jax.named_scope("p1fin"):
        finish(13)
        partner(1)
    with jax.named_scope("y1fin"):
        finish(17)
        partner(6)
    with jax.named_scope("p3fin"):
        finish(15)
        partner(3)
    with jax.named_scope("wave3"):
        wave_in(3).wait_recv()
        own(8)
    with jax.named_scope("p2fin"):
        finish(14, 0)
        partner(2, (1,3))
        finish(14, 1)
        partner(2, (2,))
    with jax.named_scope("relay7"):
        relay(7)
    with jax.named_scope("fw0"):
        finish_wave(0)
    with jax.named_scope("wave4"):
        wave_in(4).wait_recv()
        own(9)
    with jax.named_scope("from"):
        bytes_in(rt.at[1 - c], half_sem.at[0])
    with jax.named_scope("b01F"):
        blocks((0,1,), far)
    with jax.named_scope("relay8"):
        relay(8)
    with jax.named_scope("b01N"):
        blocks((0,1,), near)
    with jax.named_scope("relay9"):
        relay(9)
    with jax.named_scope("fw1"):
        finish_wave(1)
    with jax.named_scope("b2F"):
        blocks((2,), far)
    with jax.named_scope("b2N"):
        blocks((2,), near)
    with jax.named_scope("fw2"):
        finish_wave(2)
    with jax.named_scope("b3F"):
        blocks((3,), far)
    with jax.named_scope("fw3"):
        finish_wave(3)
    with jax.named_scope("b4F"):
        blocks((4,), far)
    with jax.named_scope("b34N"):
        blocks((3,4,), near)

    with jax.named_scope("density"):
        for k in range(NK):
            dsend[k : k + 1, :] = jnp.sum(dpart[k], axis=0, keepdims=True)
        dslot[band] = dsend[...]
        for d in range(1, 16):
            density_copy(d).start()

    with jax.named_scope("drain"):
        bytes_out(wave.at[:, pl.ds(0, 640)], out_sem.at[PARTNER_WAVE])
        bytes_out(wave.at[:, pl.ds(0, 1280)], out_sem.at[FAR_WAVE])
        bytes_out(w.at[0, pl.ds(0, 192)], out_sem.at[SCATTER])
        bytes_out(stage.at[pl.ds(0, 3)], out_sem.at[SPREAD])
        bytes_out(w.at[:, pl.ds(0, 1536)], out_sem.at[RING_X])
        bytes_out(w.at[:, pl.ds(0, 1536)], out_sem.at[RING_YZ])
        bytes_out(rt.at[c], out_sem.at[CORE])
        bytes_out(occ_rows.at[pl.ds(0, 3)], out_sem.at[OCC])

    with jax.named_scope("density_in"):
        bytes_in(dslot.at[pl.ds(0, 15)], in_sem.at[DENSITY])
        for g in range(4):
            total = dslot[g] + dslot[4 + g] + dslot[8 + g] + dslot[12 + g]
            dens[g * NK : (g + 1) * NK, :] = total[:NK] * (1.0 / NB)

    with jax.named_scope("out_in"):
        bytes_in(out.at[:, pl.ds(0, 1920)], in_sem.at[RESULT])
        few = out.at[:, pl.ds(0, 640)]
        pltpu.make_async_copy(few, few, in_sem.at[OWN_RESULT]).wait()
    with jax.named_scope("out_sent"):
        bytes_out(out.at[:, pl.ds(0, 1920)], out_sem.at[RESULT])
        bytes_out(dslot.at[pl.ds(0, 15)], out_sem.at[DENSITY])


def store(rotated, density, rotated_out, density_out, sem):
    copies = [pltpu.make_async_copy(density, density_out, sem.at[8])]
    for i in range(8):
        rows = pl.ds(i * 32, 32)
        copies.append(
            pltpu.make_async_copy(rotated.at[rows], rotated_out.at[rows], sem.at[i])
        )
    for copy in copies:
        copy.start()
    for copy in copies:
        copy.wait()


def per_device(wave, ritz, occupation):
    wave, ritz, occ = (
        pltpu.with_memory_space_constraint(a, pltpu.HBM)
        for a in (wave, ritz, occupation.reshape(1, 256))
    )
    dma = pltpu.SemaphoreType.DMA
    vmem = pl.BlockSpec(memory_space=pltpu.VMEM)
    anywhere = pl.BlockSpec(memory_space=pl.ANY)
    rotated, density = pl.pallas_call(
        kernel,
        out_shape=(
            jax.ShapeDtypeStruct((256, 2560), BF16),
            jax.ShapeDtypeStruct((20, 128), F32),
        ),
        in_specs=[pl.BlockSpec(memory_space=pltpu.HBM)] * 3,
        out_specs=(anywhere, vmem),
        scratch_shapes=[
            pltpu.VMEM((256, 512), BF16),
            pltpu.VMEM((1, 256), F32),
            pltpu.VMEM((2, 4, 4, 16, 256), BF16),
            pltpu.VMEM((4, 4, 16, 512), BF16),
            pltpu.VMEM((2, 4, 4, 4, 16, 2048), BF16),
            pltpu.VMEM((2, 2048, 640), BF16),
            pltpu.VMEM((NK, 4, 256, 128), BF16),
            pltpu.VMEM((4, 8, 256), F32),
            pltpu.VMEM((4, 256, 128), F32),
            pltpu.VMEM((NK, 8, 128), F32),
            pltpu.VMEM((8, 128), F32),
            pltpu.VMEM((16, 8, 128), F32),
            dma((11,)), dma((11,)), dma((NK,)), dma((28,)), dma((6,)),
        ],
        compiler_params=pltpu.CompilerParams(
            has_side_effects=True, collective_id=0, vmem_limit_bytes=VM
        ),
        name="rotate",
    )(wave, ritz, occ)
    rotated, density = pl.pallas_call(
        store,
        out_shape=(
            jax.ShapeDtypeStruct((256, 2560), BF16),
            jax.ShapeDtypeStruct((20, 128), F32),
        ),
        in_specs=[anywhere, anywhere],
        out_specs=[pl.BlockSpec(memory_space=pltpu.HBM)] * 2,
        scratch_shapes=[dma((9,))],
        compiler_params=pltpu.CompilerParams(vmem_limit_bytes=1024 * 1024),
        name="store",
    )(rotated, density)
    return rotated, density.reshape(2560)


def solution(mesh):
    return jax.shard_map(
        per_device,
        mesh=mesh,
        in_specs=(P("band", "grid"), P("band", "grid"), P("band")),
        out_specs=(P("band", "grid"), P("grid")),
        check_vma=False,
    )
```

```python
import jax
import jax.numpy as jnp
from jax import lax
from jax.experimental import pallas as pl
from jax.experimental.pallas import tpu as pltpu
from jax.sharding import PartitionSpec as P

NB = 4096
MESH = pl.DeviceIdType.MESH
F32, BF16 = jnp.float32, jnp.bfloat16

VM = 24 * 1024 * 1024
NK = 5
CA = 1408

N_RINGS = 18

PARTNER_WAVE, FAR_WAVE, SCATTER, SPREAD, RING_X, RING_YZ, CORE, OCC, RESULT, DENSITY, LOCAL = range(11)
OWN_RESULT, RITZ, OCC_HERE = RING_X, RING_YZ, CORE

def hops(*steps):
    return sum(min(step, 4 - step) for step in steps)


IN_PLANE = sorted(
    ((hops(dy, dz), dy, dz) for dy in range(4) for dz in range(4) if dy or dz),
    key=lambda d: -d[0],
)
SHARERS = [
    (hops(dx, dy), dx, dy, dc)
    for dx in range(4) for dy in (0, 2) for dc in range(2)
    if (dx, dy, dc) not in ((0, 0, 0), (0, 2, 0))
]


def at(x, y, z, core):
    return (x * 4 + (y // 2) * 2 + core, (y % 2) * 4 + z)


def kernel(
    wave, ritz, occ, out, dens,
    ritz_here, occ_here, rt_src, stage, rt, w, cbuf, occ_rows, occ_cols, dpart, dsend, dslot,
    out_sem, in_sem, wave_sem, ring_sem, half_sem,
):
    band, grid = lax.axis_index("band"), lax.axis_index("grid")
    x, yhi, c = band // 4, (band // 2) % 2, band % 2
    ylo, z = grid // 4, grid % 4
    y = yhi * 2 + ylo
    xj = 2 * ylo + z // 2
    zb = z % 2
    mine = yhi * 2 + c
    near, far = yhi, 1 - yhi

    def many(n, i):
        return pl.ds(pl.multiple_of(i * n, n), n)

    def send(src, dst, send_sem, recv_sem, device):
        return pltpu.make_async_remote_copy(
            src_ref=src, dst_ref=dst, send_sem=send_sem, recv_sem=recv_sem,
            device_id=device, device_id_type=MESH,
        )

    def cells(k):
        return pl.ds(k * 128, 128)

    def wave_local():
        return pltpu.make_async_copy(
            wave.at[:, many(640, yhi * 2 + c)], w.at[c, many(256, x * 2 + near)], in_sem.at[LOCAL]
        )

    def wave_partner(p):
        first, n = ((0, 128), (128, 512))[p]
        col = pl.multiple_of((yhi * 2 + 1 - c) * 640 + first, 128)
        return send(
            wave.at[:, pl.ds(col, n)], w.at[c, many(256, x * 2 + near), pl.ds(first, n)],
            out_sem.at[PARTNER_WAVE], half_sem.at[1] if p else in_sem.at[PARTNER_WAVE],
            at(x, y, z, 1 - c),
        )

    def wave_far(k, core):
        col = pl.multiple_of((1 - yhi) * 1280 + core * 640 + k * 128, 128)
        return send(
            wave.at[:, pl.ds(col, 128)],
            w.at[c, many(256, x * 2 + near), cells(k)],
            out_sem.at[FAR_WAVE], wave_sem.at[k], at(x, (y + 2) % 4, z, core),
        )

    def wave_in(k):
        rows = w.at[:, many(256, x * 2 + far), cells(k)]
        return send(rows, rows, out_sem.at[FAR_WAVE], wave_sem.at[k], at(x, (y + 2) % 4, z, c))

    def scatter(dy, dz):
        yp, zp = (y + dy) % 4, (z + dz) % 4
        return send(
            rt_src.at[:, zp, yp],
            stage.at[xj, many(2, zb), :, many(256, yhi)],
            out_sem.at[SCATTER], in_sem.at[SCATTER], at(x, yp, zp, c),
        )

    def spread(d):
        other = (x + d) % 4
        return send(
            stage.at[other], rt.at[c, :, z, y, :, many(512, x)],
            out_sem.at[SPREAD], in_sem.at[SPREAD], at(other, y, z, c),
        )

    def ring(i):
        if i < 10:
            k, rows = i % 5, (near if i < 5 else far)
            block = lambda v, h: w.at[h, many(256, v * 2 + rows), cells(k)]
        elif i == 10:
            block = lambda v, h: rt.at[c, pl.ds(h * 2, 2), z, v, :, pl.ds(0, CA)]
        elif i == 11:
            block = lambda v, h: rt.at[c, pl.ds(h * 2, 2), v, y, :, pl.ds(CA, 2048 - CA)]
        elif i < 16:
            block = lambda v, h: rt.at[c, pl.ds(h * 2, 2), v, (y + i - 12) % 4, :, pl.ds(0, CA)]
        else:
            n = 2048 - CA
            block = lambda v, h: rt.at[c, pl.ds((i - 16) * 2, 2), pl.ds(h * 2, 2), v, :, pl.ds(CA, n)]
        return block

    def sem_of(i, n):
        if n == 2:
            return 26 + (i == 14)
        return i if i < 10 else 10 + (i - 10) * 2 + n

    def ring_copy(i, j, v, h):
        block, slot = ring(i), i
        axis = "x" if i < 10 else "y" if i in (10, 16, 17) else "z"
        to = 1 if j < 3 else 3
        if axis == "x":
            me, device = x, at((x + to) % 4, y, z, c)
        elif axis == "y":
            me, device = y, at(x, (y + to) % 4, z, c)
        else:
            me, device = z, at(x, y, (z + to) % 4, c)
        ref = block((me + v) % 4, h)
        sent = out_sem.at[RING_X if axis == "x" else RING_YZ]
        if j in (0, 3):
            got = ring_sem.at[sem_of(slot, 0)]
        elif axis == "x":
            got = half_sem.at[2 + max(slot % 5 - 1, 0)]
        else:
            got = ring_sem.at[sem_of(slot, 2 if slot in (10, 14) and j in (2, 5) else 1)]
        return send(ref, ref, sent, got, device)

    def own_first(i):
        ring_copy(i, 0, 0, 0).start()
        ring_copy(i, 3, 0, 1).start()

    def own_rest(i):
        ring_copy(i, 1, 0, 1).start()
        ring_copy(i, 4, 0, 0).start()

    def own(i):
        own_first(i)
        own_rest(i)

    def relay(i):
        if i < 10:
            ref = rt.at[0, 0, 0, pl.ds(0, 2)]
        elif i in (16, 17):
            ref = rt.at[c, pl.ds(0, 2), :, 0, :, pl.ds(CA, 2048 - CA)]
        else:
            ref = rt.at[c, :, 0, 0, :, pl.ds(CA, 2048 - CA) if i == 11 else pl.ds(0, CA)]
        bytes_in(ref, ring_sem.at[sem_of(i, 0)])
        ring_copy(i, 2, 3, 0).start()
        ring_copy(i, 5, 1, 1).start()

    def bytes_in(ref, sem):
        send(ref, ref, out_sem.at[0], sem, at(x, y, z, 1 - c)).wait_recv()

    def bytes_out(ref, sem):
        send(ref, ref, sem, in_sem.at[0], at(x, y, z, 1 - c)).wait_send()

    def finish(i, part=0):
        low, high = pl.ds(0, CA), pl.ds(CA, 2048 - CA)
        if i in (10, 14):
            bytes_in(rt.at[c, :, 0, 0, :, low], ring_sem.at[sem_of(i, 1 + part)])
        elif i == 11:
            bytes_in(rt.at[c, :, pl.ds(0, 2), 0, :, high], ring_sem.at[sem_of(i, 1)])
        elif i < 16:
            bytes_in(rt.at[c, :, pl.ds(0, 2), 0, :, low], ring_sem.at[sem_of(i, 1)])
        else:
            bytes_in(rt.at[c, pl.ds(0, 2), :, pl.ds(0, 2), :, high], ring_sem.at[sem_of(i, 1)])

    def finish_wave(g):
        bytes_in(rt.at[0, 0, pl.ds(0, 2 if g else 4)], half_sem.at[2 + g])

    def to_core(ref, sem):
        send(ref, ref, out_sem.at[CORE], half_sem.at[sem], at(x, y, z, 1 - c)).start()

    def partner(half, d, vs=None):
        for v in vs or (None,):
            planes = slice(None) if v is None else (z + v) % 4
            to_core(
                rt.at[c, many(2, half), planes, (y + d) % 4, :, pl.ds(0, CA)], 6 if half is near else 0
            )

    def partner_rest(half, ds):
        for d in ds:
            ref = rt.at[c, pl.ds(half * 2, 2), :, (y + d) % 4, :, pl.ds(CA, 2048 - CA)]
            to_core(ref, ((half + far) % 2) * 6)

    def occ_copy(d, src=False):
        yy = y if d == 0 else (y + 2) % 4
        cc = c if d == 1 else 1 - c
        row = (yy // 2) * 2 + cc if src else mine
        return send(
            occ_rows.at[mine], occ_rows.at[row], out_sem.at[OCC], in_sem.at[OCC], at(x, yy, z, cc)
        )

    def result(k, hi, core):
        return send(
            cbuf.at[k, hi * 2 + core], out.at[:, many(128, yhi * 10 + c * 5 + k)],
            out_sem.at[RESULT], in_sem.at[RESULT], at(x, hi * 2 + ylo, z, core),
        )

    def result_here(k):
        return pltpu.make_async_copy(
            cbuf.at[k, mine], out.at[:, many(128, yhi * 10 + c * 5 + k)], in_sem.at[OWN_RESULT]
        )

    def density_copy(d):
        to = at((x + d // 4) % 4, (y + 2 * ((d // 2) % 2)) % 4, z, (c + d) % 2)
        return send(dsend, dslot.at[band], out_sem.at[DENSITY], in_sem.at[DENSITY], to)

    def take(k, s, summed):
        rounded = summed.astype(BF16)
        cbuf[k, s] = rounded
        values = rounded.astype(F32)
        terms = occ_cols[s] * values * values
        dpart[k] += terms.reshape(32, 8, 128).sum(axis=0)

    def product(s, ks):
        cols = pl.ds(ks[0] * 128, 128 * len(ks))
        parts = [
            jnp.dot(
                rt[v, s].reshape(256, 2048), w[v, :, cols], preferred_element_type=F32
            )
            for v in range(2)
        ]
        return parts[0] + parts[1]

    def blocks(ks, hi):
        @pl.loop(0, 2)
        def _(core):
            s = hi * 2 + core
            summed = product(s, ks)
            for n, k in enumerate(ks):
                take(k, s, summed[:, n * 128 : (n + 1) * 128])
            if hi is far:
                for k in ks:
                    result(k, hi, core).start()

        if hi is near:
            for k in ks:
                result(k, hi, 1 - c).start()
            for k in ks:
                result_here(k).start()

    with jax.named_scope("signal"):
        peers = [(n, at((x + dx) % 4, (y + dy) % 4, z, (c + dc) % 2)) for n, dx, dy, dc in SHARERS]
        peers += [(n, at(x, (y + dy) % 4, (z + dz) % 4, c)) for n, dy, dz in IN_PLANE]
        peers = [peer for _, peer in sorted(peers, key=lambda p: -p[0])]
        barrier = pltpu.get_barrier_semaphore()
        for peer in peers:
            pl.semaphore_signal(barrier, inc=1, device_id=peer, device_id_type=MESH)
        load_ritz = pltpu.make_async_copy(ritz, ritz_here, in_sem.at[RITZ])
        load_occ = pltpu.make_async_copy(occ, occ_here, in_sem.at[OCC_HERE])
        load_ritz.start()
        load_occ.start()
        wave_local().start()

    with jax.named_scope("transpose"):
        load_ritz.wait()
        load_occ.wait()
        rt_src[...] = ritz_here[...].T.reshape(2, 4, 4, 16, 256)
        occ_rows[mine] = jnp.broadcast_to(occ_here[...], (8, 256))
        stage[xj, many(2, zb), :, many(256, yhi)] = rt_src[:, z, y]
        dpart[...] = jnp.zeros_like(dpart)
        dsend[...] = jnp.zeros_like(dsend)
    with jax.named_scope("barrier"):
        pl.semaphore_wait(barrier, len(peers))

    with jax.named_scope("start"):
        for _, dy, dz in IN_PLANE:
            scatter(dy, dz).start()
        wave_local().wait()
        for p in range(2):
            wave_partner(p).start()
        for d in range(3):
            occ_copy(d).start()
    with jax.named_scope("pw"):
        bytes_in(wave.at[:, pl.ds(0, 128)], in_sem.at[PARTNER_WAVE])
        own(0)
        bytes_in(wave.at[:, pl.ds(0, 512)], half_sem.at[1])
    with jax.named_scope("scin"):
        bytes_in(w.at[0, pl.ds(0, 192)], in_sem.at[SCATTER])
        for d in (2, 1, 3):
            spread(d).start()
        rt[c, :, z, y, :, many(512, x)] = stage[x]
        for core in range(2):
            wave_far(0, core).start()
        for core in range(2):
            wave_far(1, core).start()
        own(1)
        own(2)
        own(3)
        own(4)
    with jax.named_scope("spin"):
        bytes_in(stage.at[pl.ds(0, 3)], in_sem.at[SPREAD])
        own(11)
        own(12)
        own(10)
    with jax.named_scope("occ"):
        bytes_in(occ_rows.at[pl.ds(0, 3)], in_sem.at[OCC])
        for s in range(4):
            occ_cols[s] = jnp.broadcast_to(occ_rows[s][0:1, :], (128, 256)).T
    with jax.named_scope("s1relay"):
        relay(10)
        relay(11)
        for core in range(2):
            wave_far(2, core).start()
    with jax.named_scope("relay0"):
        relay(0)
    with jax.named_scope("wave0"):
        wave_in(0).wait_recv()
        own(5)
    with jax.named_scope("finA"):
        finish(10, 0)
        own(13)
        own(15)
    with jax.named_scope("z1fin"):
        finish(11)
        own(16)
        own(17)
        partner_rest(0, (0,))
        partner_rest(1, (0,))
    with jax.named_scope("p0relay"):
        relay(12)
    with jax.named_scope("s1fin"):
        finish(10, 1)
        own(14)
        partner(far, 2, (0,))
        partner(near, 2, (0,))
    with jax.named_scope("relay1"):
        relay(1)
    with jax.named_scope("y0relay"):
        relay(16)
    with jax.named_scope("relay2"):
        relay(2)
    with jax.named_scope("wave1"):
        wave_in(1).wait_recv()
        own(6)
    with jax.named_scope("y1relay"):
        relay(17)
        for core in range(2):
            wave_far(3, core).start()
        for core in range(2):
            wave_far(4, core).start()
    with jax.named_scope("relay3"):
        relay(3)
    with jax.named_scope("relay5"):
        relay(5)
    with jax.named_scope("p1relay"):
        relay(13)
    with jax.named_scope("p0fin"):
        finish(12)
        partner(far, 0)
        partner(near, 0)
    with jax.named_scope("y0fin"):
        finish(16)
        partner_rest(0, (1,2,3))
    with jax.named_scope("p3relay"):
        relay(15)
    with jax.named_scope("relay4"):
        relay(4)
    with jax.named_scope("p2relay"):
        relay(14)
    with jax.named_scope("relay6"):
        relay(6)
    with jax.named_scope("wave2"):
        wave_in(2).wait_recv()
        own(7)
    with jax.named_scope("p1fin"):
        finish(13)
        partner(far, 1)
        partner(near, 1)
    with jax.named_scope("y1fin"):
        finish(17)
        partner_rest(1, (1,2,3))
    with jax.named_scope("p3fin"):
        finish(15)
        partner(far, 3)
    with jax.named_scope("wave3"):
        wave_in(3).wait_recv()
        own(8)
    with jax.named_scope("p2fin"):
        finish(14, 0)
        partner(far, 2, (1,3))
        finish(14, 1)
        partner(far, 2, (2,))
        partner(near, 3)
        partner(near, 2, (1,2,3))
    with jax.named_scope("relay7"):
        relay(7)
    with jax.named_scope("fw0"):
        finish_wave(0)
    with jax.named_scope("wave4"):
        wave_in(4).wait_recv()
        own(9)
    with jax.named_scope("from"):
        bytes_in(rt.at[1 - c, pl.ds(0, 2)], half_sem.at[0])
    with jax.named_scope("b01F"):
        blocks((0,), far)
        blocks((1,), far)
    with jax.named_scope("relay8"):
        relay(8)
    with jax.named_scope("fromN"):
        bytes_in(rt.at[1 - c, pl.ds(0, 2)], half_sem.at[6])
    with jax.named_scope("b01N"):
        blocks((0,1,), near)
    with jax.named_scope("fw1"):
        finish_wave(1)
    with jax.named_scope("b2F"):
        blocks((2,), far)
    with jax.named_scope("relay9"):
        relay(9)
    with jax.named_scope("b2N"):
        blocks((2,), near)
    with jax.named_scope("fw2"):
        finish_wave(2)
    with jax.named_scope("b3F"):
        blocks((3,), far)
    with jax.named_scope("fw3"):
        finish_wave(3)
    with jax.named_scope("b4F"):
        blocks((4,), far)
    with jax.named_scope("b34N"):
        blocks((3,4,), near)

    with jax.named_scope("density"):
        for k in range(NK):
            dsend[k : k + 1, :] = jnp.sum(dpart[k], axis=0, keepdims=True)
        dslot[band] = dsend[...]
        for d in range(1, 16):
            density_copy(d).start()

    with jax.named_scope("drain"):
        bytes_out(wave.at[:, pl.ds(0, 640)], out_sem.at[PARTNER_WAVE])
        bytes_out(wave.at[:, pl.ds(0, 1280)], out_sem.at[FAR_WAVE])
        bytes_out(w.at[0, pl.ds(0, 192)], out_sem.at[SCATTER])
        bytes_out(stage.at[pl.ds(0, 3)], out_sem.at[SPREAD])
        bytes_out(w.at[:, pl.ds(0, 1536)], out_sem.at[RING_X])
        bytes_out(w.at[:, pl.ds(0, 1536)], out_sem.at[RING_YZ])
        bytes_out(rt.at[c], out_sem.at[CORE])
        bytes_out(occ_rows.at[pl.ds(0, 3)], out_sem.at[OCC])

    with jax.named_scope("density_in"):
        bytes_in(dslot.at[pl.ds(0, 15)], in_sem.at[DENSITY])
        for g in range(4):
            total = dslot[g] + dslot[4 + g] + dslot[8 + g] + dslot[12 + g]
            dens[g * NK : (g + 1) * NK, :] = total[:NK] * (1.0 / NB)

    with jax.named_scope("out_in"):
        bytes_in(out.at[:, pl.ds(0, 1920)], in_sem.at[RESULT])
        few = out.at[:, pl.ds(0, 640)]
        pltpu.make_async_copy(few, few, in_sem.at[OWN_RESULT]).wait()
    with jax.named_scope("out_sent"):
        bytes_out(out.at[:, pl.ds(0, 1920)], out_sem.at[RESULT])
        bytes_out(dslot.at[pl.ds(0, 15)], out_sem.at[DENSITY])


def store(rotated, density, rotated_out, density_out, sem):
    copies = [pltpu.make_async_copy(density, density_out, sem.at[8])]
    for i in range(8):
        rows = pl.ds(i * 32, 32)
        copies.append(
            pltpu.make_async_copy(rotated.at[rows], rotated_out.at[rows], sem.at[i])
        )
    for copy in copies:
        copy.start()
    for copy in copies:
        copy.wait()


def per_device(wave, ritz, occupation):
    wave, ritz, occ = (
        pltpu.with_memory_space_constraint(a, pltpu.HBM)
        for a in (wave, ritz, occupation.reshape(1, 256))
    )
    dma = pltpu.SemaphoreType.DMA
    vmem = pl.BlockSpec(memory_space=pltpu.VMEM)
    anywhere = pl.BlockSpec(memory_space=pl.ANY)
    rotated, density = pl.pallas_call(
        kernel,
        out_shape=(
            jax.ShapeDtypeStruct((256, 2560), BF16),
            jax.ShapeDtypeStruct((20, 128), F32),
        ),
        in_specs=[pl.BlockSpec(memory_space=pltpu.HBM)] * 3,
        out_specs=(anywhere, vmem),
        scratch_shapes=[
            pltpu.VMEM((256, 512), BF16),
            pltpu.VMEM((1, 256), F32),
            pltpu.VMEM((2, 4, 4, 16, 256), BF16),
            pltpu.VMEM((4, 4, 16, 512), BF16),
            pltpu.VMEM((2, 4, 4, 4, 16, 2048), BF16),
            pltpu.VMEM((2, 2048, 640), BF16),
            pltpu.VMEM((NK, 4, 256, 128), BF16),
            pltpu.VMEM((4, 8, 256), F32),
            pltpu.VMEM((4, 256, 128), F32),
            pltpu.VMEM((NK, 8, 128), F32),
            pltpu.VMEM((8, 128), F32),
            pltpu.VMEM((16, 8, 128), F32),
            dma((11,)), dma((11,)), dma((NK,)), dma((28,)), dma((7,)),
        ],
        compiler_params=pltpu.CompilerParams(
            has_side_effects=True, collective_id=0, vmem_limit_bytes=VM,
        ),
        name="rotate",
    )(wave, ritz, occ)
    rotated, density = pl.pallas_call(
        store,
        out_shape=(
            jax.ShapeDtypeStruct((256, 2560), BF16),
            jax.ShapeDtypeStruct((20, 128), F32),
        ),
        in_specs=[anywhere, anywhere],
        out_specs=[pl.BlockSpec(memory_space=pltpu.HBM)] * 2,
        scratch_shapes=[dma((9,))],
        compiler_params=pltpu.CompilerParams(vmem_limit_bytes=1024 * 1024),
        name="store",
    )(rotated, density)
    return rotated, density.reshape(2560)


def solution(mesh):
    return jax.shard_map(
        per_device,
        mesh=mesh,
        in_specs=(P("band", "grid"), P("band", "grid"), P("band")),
        out_specs=(P("band", "grid"), P("grid")),
        check_vma=False,
    )
```
